128 devices in a mesh: seq: 16 (over z_hi, y, core), tensor: 8 (over z_lo, x).
Axes of the slice: x: 4, y: 4, z: 4 (z_hi: 2, z_lo: 2; z = z_hi * 2 + z_lo), core: 2. Of those that a mesh axis runs over, the one named last changes fastest.
Arguments:
- tokens: bfloat16 [11520, 1536], P('seq'), may hold values from -6 to 6
- norm_gain: float32 [1536], replicated, may hold values from 0.1 to 1.9
- w_qkv: bfloat16 [1536, 3, 1536], P(None, None, 'tensor'), may hold values from -8 to 8
- w_out: bfloat16 [1536, 1536], P('tensor'), may hold values from -0.15625 to 0.15625
- post_gain: float32 [1536], replicated, may hold values from 0.1 to 1.9
- w_up: bfloat16 [1536, 6144], P(None, 'tensor'), may hold values from -0.15625 to 0.15625
- w_down: bfloat16 [6144, 1536], P('tensor'), may hold values from -0.078125 to 0.078125
Outputs:
- layer_out: bfloat16 [11520, 1536], P('seq')
The draws below stay inside these ranges and needn't reach their ends.
All inputs are finite; a program needn't handle non-finite values.
Results may differ from the reference program's by a relative error of at most 0.015.
Values may be sent and summed in bfloat16 or wider, within the bound.
A program may use at most 128 MiB of HBM per device.

```python
import math
import jax
import jax.numpy as jnp
from jax import lax

D = 1536
HEADS = 32
HD = 48
FF = 6144
TOK_DEV = 720
TOKENS = 11520
N_TENSOR = 8


def draw_w_qkv(key, part):
    base = jax.random.normal(key, (D, 3, HEADS * HD), jnp.float32) * D ** (-0.5)
    levels = jax.random.uniform(jax.random.fold_in(key, 3), (HEADS,), jnp.float32, math.log(1.5), math.log(3.5))
    sharpness = jnp.repeat(jnp.exp(levels), HD)
    query = base[:, 0, :] * sharpness[None, :]
    stacked = jnp.stack([query, base[:, 1, :], base[:, 2, :]], axis=1)
    return jnp.clip(stacked, -8.0, 8.0).astype(jnp.bfloat16)


def level_of(stream_key, shape, cuts, least, top_value):
    def one(dim, parts):
        steps = jax.random.uniform(jax.random.fold_in(jax.random.fold_in(stream_key, 6), dim), (parts,), jnp.float32, least / len(cuts), top_value / len(cuts))
        return jnp.repeat(jnp.exp(steps), shape[dim] // parts).reshape((-1,) + (1,) * (len(shape) - dim - 1))

    level = one(*cuts[0])
    for cut in cuts[1:]:
        level = level * one(*cut)
    return level


def scatter_about(rng, extent, scale, bound, split=(), dtype=jnp.bfloat16):
    loudness = level_of(rng, extent, split, -0.22, 0.18) if split else 1.0
    array = jax.random.normal(rng, extent, jnp.float32) * scale * loudness
    return jnp.minimum(jnp.maximum(array, -bound), bound).astype(dtype)


def setup_inputs(seed: int = 0) -> dict:
    key_list = jax.random.split(jax.random.key(seed), 8)
    return {
        "tokens": scatter_about(key_list[0], (TOKENS, D), 1.0, 6.0, ((0, 16),)),
        "norm_gain": jnp.clip(1.0 + 0.18 * jax.random.normal(key_list[1], (D,), jnp.float32), 0.1, 1.9),
        "w_qkv": draw_w_qkv(jax.random.fold_in(key_list[7], 71), 0),
        "w_out": scatter_about(key_list[3], (HEADS * HD, D), (HEADS * HD) ** -0.5, 0.15625, ((0, 8),)),
        "post_gain": jnp.clip(1.0 + 0.18 * jax.random.normal(key_list[4], (D,), jnp.float32), 0.1, 1.9),
        "w_up": scatter_about(key_list[5], (D, FF), D ** -0.5, 0.15625, ((1, 8),)),
        "w_down": scatter_about(key_list[6], (FF, D), FF ** -0.5, 0.078125, ((0, 8),)),
    }


def layer_norm(values, gain):
    mean = lax.optimization_barrier(jnp.mean(values, axis=-1, keepdims=True))
    centred = values - mean
    var = lax.optimization_barrier(jnp.mean(centred * centred, axis=-1, keepdims=True))
    return centred * lax.rsqrt(var + 1e-05) * gain

def one_head(operands):
    query, key, value = operands
    scale = 1.0 / HD ** 0.5

    def block(query_block):
        scores = jnp.dot(query_block, key.T, preferred_element_type=jnp.float32) * scale
        peak = lax.optimization_barrier(jnp.max(scores, axis=-1, keepdims=True))
        weights = jnp.exp(scores - peak)
        total = lax.optimization_barrier(jnp.sum(weights, axis=-1, keepdims=True))
        return jnp.dot(weights.astype(jnp.bfloat16), value, preferred_element_type=jnp.float32) / total
    blocks = query.reshape(TOKENS // TOK_DEV, TOK_DEV, HD)
    return lax.map(block, blocks).reshape(TOKENS, HD)

def grouped_sum(left, right):
    width = left.shape[1] // N_TENSOR
    result = jnp.zeros((left.shape[0], right.shape[1]), jnp.float32)
    for group in range(N_TENSOR):
        term = jnp.dot(left[:, group * width:(group + 1) * width], right[group * width:(group + 1) * width], preferred_element_type=jnp.float32)
        term = lax.optimization_barrier(term.astype(jnp.bfloat16))
        result = result + term.astype(jnp.float32)
    return result

def reference(tokens, norm_gain, w_qkv, w_out, post_gain, w_up, w_down):
    base = tokens.astype(jnp.float32)
    normed = layer_norm(base, norm_gain).astype(jnp.bfloat16)
    qkv = jnp.dot(normed, w_qkv.reshape(D, 3 * HEADS * HD), preferred_element_type=jnp.float32).astype(jnp.bfloat16)
    qkv = qkv.reshape(TOKENS, 3, HEADS, HD)
    query = jnp.transpose(qkv[:, 0], (1, 0, 2))
    key = jnp.transpose(qkv[:, 1], (1, 0, 2))
    value = jnp.transpose(qkv[:, 2], (1, 0, 2))
    heads = lax.map(one_head, (query, key, value))
    attended = jnp.transpose(heads, (1, 0, 2)).reshape(TOKENS, HEADS * HD).astype(jnp.bfloat16)
    mixed = base + grouped_sum(attended, w_out)
    post = layer_norm(mixed, post_gain).astype(jnp.bfloat16)
    hidden = jax.nn.gelu(jnp.dot(post, w_up, preferred_element_type=jnp.float32), approximate=True).astype(jnp.bfloat16)
    return (mixed + grouped_sum(hidden, w_down)).astype(jnp.bfloat16)
```

```python
import functools

import jax
import jax.numpy as jnp
from jax import lax
from jax.experimental import pallas as pl
from jax.experimental.pallas import tpu as pltpu
from jax.sharding import PartitionSpec as P

HD = 48
ROWS = 720
PAD = 768
NSEQ = 16
NTEN = 8
W = 256
NC = PAD // W
f32 = jnp.float32
bf16 = jnp.bfloat16
MESH = pl.DeviceIdType.MESH

OWN, A, B, C, F, D, E, G = range(8)
DZ = (0, 0, 0, 1, 0, 1, 1, 1)
DY = (0, 3, 1, 0, 2, 3, 1, 2)
ORDER = (
    (OWN, 0), (OWN, 1), (A, 0), (B, 0), (C, 0), (A, 1), (B, 1), (C, 1),
    (F, 0), (F, 1), (D, 0), (E, 0), (D, 1), (E, 1), (G, 0), (G, 1),
)
ARRIVE = {0: ((OWN, 1),), 1: ((A, 0), (B, 0), (C, 0)), 4: ((A, 1),), 5: ((B, 1),), 6: ((C, 1),), 7: ((F, 0),), 8: ((F, 1),),
          9: ((D, 0), (E, 0)), 11: ((D, 1),), 12: ((E, 1),), 13: ((G, 0),), 14: ((G, 1),)}


def layer_norm(values, gain):
    mean = jnp.mean(values, axis=-1, keepdims=True)
    centred = values - mean
    var = jnp.mean(centred * centred, axis=-1, keepdims=True)
    return centred * lax.rsqrt(var + 1e-05) * gain


def attention_kernel(qkv, out, kt, vt, s0, s1, p0, p1, acc, peak, ssem, rsem, tsend, trecv):
    me = lax.axis_index("seq")
    ti = lax.axis_index("tensor")
    zh, yy, core = lax.div(me, 8), lax.rem(lax.div(me, 2), 4), lax.rem(me, 2)
    zl, xx = lax.div(ti, 4), lax.rem(ti, 4)

    def seq_id(off, other=0):
        return (lax.rem(zh + DZ[off], 2) * 4 + lax.rem(yy + DY[off], 4)) * 2 + lax.rem(core + other, 2)

    def ten_id(dz, dx):
        return lax.rem(zl + dz, 2) * 4 + lax.rem(xx + dx, 4)

    seq_near = [seq_id(OWN, 1), seq_id(A), seq_id(B), seq_id(C)]
    ten_near = [ten_id(0, 1), ten_id(0, 3), ten_id(1, 0), ten_id(1, 1), ten_id(1, 3)]
    barrier = pltpu.get_barrier_semaphore()
    for d in seq_near:
        pl.semaphore_signal(barrier, inc=1, device_id={"seq": d}, device_id_type=MESH)
    for d in ten_near:
        pl.semaphore_signal(barrier, inc=1, device_id={"tensor": d}, device_id_type=MESH)

    lane = lax.broadcasted_iota(jnp.int32, (16, PAD), 1)
    row = lax.broadcasted_iota(jnp.int32, (16, PAD), 0)
    ones = jnp.where((row == 0) & (lane < ROWS), 1.0, 0.0).astype(bf16)

    def fill(s, _):
        for h in range(4):
            vt[s, h, HD:64, :] = ones
        return 0

    lax.fori_loop(0, NSEQ, fill, 0)
    for h in range(4):
        kt[me, h] = qkv[1, h]
        vt[me, h, 0:HD, :] = qkv[2, h]
    peak[...] = jnp.full(peak.shape, -1e30, f32)
    acc[...] = jnp.zeros(acc.shape, f32)
    p0[ROWS:PAD, :] = jnp.zeros((PAD - ROWS, PAD), bf16)
    p1[ROWS:PAD, :] = jnp.zeros((PAD - ROWS, PAD), bf16)
    pl.semaphore_wait(barrier, len(seq_near) + len(ten_near))

    sent = [[], []]

    def block_ref(piece, slot, hp):
        ref = kt if piece == 0 else vt
        return ref.at[slot, 2 * hp : 2 * hp + 2, 0:HD]

    def seq_copy(piece, slot, hp, dest, index, own=False):
        src = qkv.at[1 + piece, 2 * hp : 2 * hp + 2] if own else block_ref(piece, slot, hp)
        return pltpu.make_async_remote_copy(
            src_ref=src, dst_ref=block_ref(piece, slot, hp), send_sem=ssem.at[hp, index],
            recv_sem=rsem.at[slot, hp, piece], device_id={"seq": dest}, device_id_type=MESH,
        )

    def send(piece, slot, hp, dest, own=False):
        c = seq_copy(piece, slot, hp, dest, len(sent[hp]), own)
        c.start()
        sent[hp].append(piece)

    def send_own(hp):
        for piece in (0, 1):
            for d in (seq_id(B), seq_id(A), seq_id(C), seq_id(OWN, 1)):
                send(piece, me, hp, d, own=True)

    def arrive(hp, off, other):
        slot = seq_id(off, other)
        for piece in (0, 1):
            seq_copy(piece, slot, hp, me, 0).wait_recv()
        if other:
            return
        if off in (A, D):
            send(0, slot, hp, seq_id(B))
        if off in (B, E):
            send(1, slot, hp, seq_id(A))
        for piece in (0, 1):
            send(piece, slot, hp, seq_id(OWN, 1))

    def spread(hp):
        slot = seq_id(C)
        for piece in (0, 1):
            for d in (seq_id(B), seq_id(A)):
                send(piece, slot, hp, d)

    tsent = []

    def ten_copy(src, head, dest, index):
        return pltpu.make_async_remote_copy(
            src_ref=out.at[src, head], dst_ref=out.at[src, head], send_sem=tsend.at[index],
            recv_sem=trecv.at[src, head], device_id={"tensor": dest}, device_id_type=MESH,
        )

    def ten_start(src, head, dest):
        c = ten_copy(src, head, dest, len(tsent))
        c.start()
        tsent.append(0)

    def finish(hp):
        for h in (2 * hp, 2 * hp + 1):
            out[ti, h] = (acc[h, 0:HD, :] / acc[h, HD : HD + 1, :]).astype(bf16)
        for h in (2 * hp, 2 * hp + 1):
            for d in ten_near:
                ten_start(ti, h, d)

    def ten_wait(src, head):
        ten_copy(src, head, ti, 0).wait_recv()

    def relay(hp):
        for dz in (0, 1):
            left, right = ten_id(dz, 3), ten_id(dz, 1)
            for h in (2 * hp, 2 * hp + 1):
                ten_wait(left, h)
                ten_wait(right, h)
            ten_start(left, 2 * hp, ten_id(0, 1))
            ten_start(right, 2 * hp + 1, ten_id(0, 3))

    def collect(hp):
        for h in (2 * hp, 2 * hp + 1):
            ten_wait(ten_id(1, 0), h)
            ten_wait(ten_id(0, 2), h)
            ten_wait(ten_id(1, 2), h)

    S, Pw = (s0, s1), (p0, p1)

    def slot_at(pos):
        code = pos * 0
        for j, (off, other) in enumerate(ORDER):
            code = code + (pos == j).astype(jnp.int32) * (DZ[off] * 8 + DY[off] * 2 + other)
        dz, dy, dc = lax.div(code, 8), lax.rem(lax.div(code, 2), 4), lax.rem(code, 2)
        return (lax.rem(zh + dz, 2) * 4 + lax.rem(yy + dy, 4)) * 2 + lax.rem(core + dc, 2)

    def score_pieces(slot, head, par, top):
        def mk(c, half):
            cs = slice(c * W, (c + 1) * W)

            def go():
                lo = half * 384
                n = 384 if half == 0 else ROWS - 384
                s = lax.dot_general(
                    kt[slot, head, :, lo : lo + 384], qkv[0, head, :, cs], (((0,), (0,)), ((), ())), preferred_element_type=f32
                )[0:n]
                S[par][lo : lo + n, cs] = s
                b = jnp.max(s.reshape(-1, 8, W), axis=0)
                top[c] = b if c not in top else jnp.maximum(top[c], b)

            return go

        return [mk(c, half) for c in range(NC) for half in (0, 1)]

    def weight_pieces(par, now):
        def mk(c, r):
            cs = slice(c * W, (c + 1) * W)

            def go():
                Pw[par][r : r + 240, cs] = jnp.exp2(S[par][r : r + 240, cs] - now[c]).astype(bf16)

            return go

        return [mk(c, r) for c in range(NC) for r in (0, 240, 480)]

    def value_pieces(slot, head, par, factor):
        def mk(c):
            cs = slice(c * W, (c + 1) * W)

            def go():
                acc[head, :, cs] = acc[head, :, cs] * factor[c] + jnp.dot(
                    vt[slot, head], Pw[par][:, cs], preferred_element_type=f32
                )

            return go

        return [mk(c) for c in range(NC)]

    def interleave(*lists):
        events = []
        for k, items in enumerate(lists):
            for j, x in enumerate(items):
                events.append(((j + 0.5) / len(items), k, x))
        events.sort(key=lambda e: (e[0], e[1]))
        for _, _, x in events:
            x()

    def keep_top(head, top):
        for c in range(NC):
            peak[head, 8:16, c * W : (c + 1) * W] = top[c]

    def step(t, _):
        for hp in (0, 1):
            for j, blocks in ARRIVE.items():

                @pl.when(t == 16 * hp + j)
                def _(hp=hp, j=j, blocks=blocks):
                    for off, other in blocks:
                        arrive(hp, off, other)
                    if j == 1:
                        spread(hp)
                    if j == 9 and hp == 0:
                        send_own(1)

        @pl.when(t == 16)
        def _():
            finish(0)

        @pl.when(t == 22)
        def _():
            relay(0)

        @pl.when(t == 28)
        def _():
            collect(0)

        hp = lax.div(t, 16)
        slot = slot_at(lax.rem(t, 16))
        nxt = lax.rem(t + 1, 32)
        slot_next = slot_at(lax.rem(nxt, 16))
        held = None
        for k in (0, 1):
            head = 2 * hp + k
            now, factor = {}, {}
            for c in range(NC):
                cs = slice(c * W, (c + 1) * W)
                old = peak[head, 0:1, cs]
                now[c] = jnp.maximum(old, jnp.max(peak[head, 8:16, cs], axis=0, keepdims=True))
                factor[c] = jnp.exp2(old - now[c])
                peak[head, 0:1, cs] = now[c]
            head_n = head + 1 if k == 0 else 2 * lax.div(nxt, 16)
            slot_n = slot if k == 0 else slot_next
            top = {}
            scores = score_pieces(slot_n, head_n, 1 - k, top)
            weights = weight_pieces(k, now)
            if held is None:
                interleave(scores, weights)
                held = value_pieces(slot, head, k, factor)
            else:
                interleave(scores, weights, held)
                for x in value_pieces(slot, head, k, factor):
                    x()
            keep_top(head_n, top)
        return 0

    send_own(0)
    top = {}
    for x in score_pieces(me, 0, 0, top):
        x()
    keep_top(0, top)
    lax.fori_loop(0, 32, step, 0)
    finish(1)
    relay(1)
    collect(1)
    for hp in (0, 1):
        for index, piece in enumerate(sent[hp]):
            seq_copy(piece, me, hp, me, index).wait_send()
    for index in range(len(tsent)):
        ten_copy(ti, 0, ti, index).wait_send()


def attention(qkv):
    vmem = pl.BlockSpec(memory_space=pltpu.VMEM)
    return pl.pallas_call(
        attention_kernel,
        out_shape=jax.ShapeDtypeStruct((NTEN, 4, HD, PAD), bf16),
        in_specs=[vmem],
        out_specs=vmem,
        scratch_shapes=[
            pltpu.VMEM((NSEQ, 4, HD, PAD), bf16),
            pltpu.VMEM((NSEQ, 4, 64, PAD), bf16),
            pltpu.VMEM((ROWS, PAD), f32),
            pltpu.VMEM((ROWS, PAD), f32),
            pltpu.VMEM((PAD, PAD), bf16),
            pltpu.VMEM((PAD, PAD), bf16),
            pltpu.VMEM((4, 64, PAD), f32),
            pltpu.VMEM((4, 16, PAD), f32),
            pltpu.SemaphoreType.DMA((2, 32)),
            pltpu.SemaphoreType.DMA((NSEQ, 2, 2)),
            pltpu.SemaphoreType.DMA((32,)),
            pltpu.SemaphoreType.DMA((NTEN, 4)),
        ],
        compiler_params=pltpu.CompilerParams(collective_id=0, has_side_effects=True, vmem_limit_bytes=48 * 2**20),
        cost_estimate=pl.CostEstimate(flops=60_000_000_000, bytes_accessed=4_000_000, transcendentals=33_000_000),
        name="attention",
    )(qkv)


def per_device(tokens, norm_gain, w_qkv, w_out, post_gain, w_up, w_down):
    w_full = lax.all_gather(w_out, "tensor", axis=0, tiled=True)
    base = tokens.astype(f32)
    normed = layer_norm(base, norm_gain).astype(bf16)
    qkv = lax.dot_general(w_qkv.reshape(w_qkv.shape[0], -1), normed, (((0,), (1,)), ((), ())), preferred_element_type=f32)
    scale = jnp.concatenate([jnp.full((192, 1), 1.4426950408889634 / HD**0.5, f32), jnp.ones((384, 1), f32)])
    qkv = jnp.pad((qkv * scale).astype(bf16), ((0, 0), (0, PAD - ROWS))).reshape(3, 4, HD, PAD)
    attended = attention(qkv).reshape(NTEN * 4 * HD, PAD)
    mixed = base + lax.dot_general(attended, w_full, (((0,), (0,)), ((), ())), preferred_element_type=f32)[:ROWS]
    post = layer_norm(mixed, post_gain).astype(bf16)
    hidden = jax.nn.gelu(jnp.dot(post, w_up, preferred_element_type=f32), approximate=True).astype(bf16)
    mlp_term = jnp.dot(hidden, w_down, preferred_element_type=f32)
    return (mixed + lax.psum(mlp_term.astype(bf16), "tensor").astype(f32)).astype(bf16)


def solution(mesh):
    placed = (P("seq", None), P(), P(None, None, "tensor"), P("tensor", None), P(), P(None, "tensor"), P("tensor", None))
    return jax.shard_map(per_device, mesh=mesh, in_specs=placed, out_specs=P("seq", None), check_vma=False)
```

```python
import functools

import jax
import jax.numpy as jnp
from jax import lax
from jax.experimental import pallas as pl
from jax.experimental.pallas import tpu as pltpu
from jax.sharding import PartitionSpec as P

HD = 48
ROWS = 720
PAD = 768
NSEQ = 16
NTEN = 8
W = 256
NC = PAD // W
f32 = jnp.float32
bf16 = jnp.bfloat16
MESH = pl.DeviceIdType.MESH

OWN, A, B, C, F, D, E, G = range(8)
DZ = (0, 0, 0, 1, 0, 1, 1, 1)
DY = (0, 3, 1, 0, 2, 3, 1, 2)
ORDER = (
    (OWN, 0), (OWN, 1), (A, 0), (B, 0), (C, 0), (A, 1), (B, 1), (C, 1),
    (F, 0), (F, 1), (D, 0), (E, 0), (D, 1), (E, 1), (G, 0), (G, 1),
)
ARRIVE = {0: ((OWN, 1),), 1: ((A, 0), (B, 0), (C, 0)), 4: ((A, 1),), 5: ((B, 1),), 6: ((C, 1),), 7: ((F, 0),), 8: ((F, 1),),
          9: ((D, 0), (E, 0)), 11: ((D, 1),), 12: ((E, 1),), 13: ((G, 0),), 14: ((G, 1),)}


def layer_norm(values, gain):
    mean = jnp.mean(values, axis=-1, keepdims=True)
    centred = values - mean
    var = jnp.mean(centred * centred, axis=-1, keepdims=True)
    return centred * lax.rsqrt(var + 1e-05) * gain


def layer_kernel(qkv, gain, tokens, w_out, w_up, w_down, out, kt, vt, s0, s1, p0, p1, acc, peak, att, wf, tok, wu, wd,
                 mixed, post, term, ra, rb, ra2, rb2, sa2, sb2, ssem, rsem, tsend, trecv, wsend, wrecv, lsem,
                 qsend, rarecv, rbrecv, ra2recv, rb2recv, gsend, grecv):
    me = lax.axis_index("seq")
    ti = lax.axis_index("tensor")
    zh, yy, core = lax.div(me, 8), lax.rem(lax.div(me, 2), 4), lax.rem(me, 2)
    zl, xx = lax.div(ti, 4), lax.rem(ti, 4)

    def seq_id(off, other=0):
        return (lax.rem(zh + DZ[off], 2) * 4 + lax.rem(yy + DY[off], 4)) * 2 + lax.rem(core + other, 2)

    def ten_id(dz, dx):
        return lax.rem(zl + dz, 2) * 4 + lax.rem(xx + dx, 4)

    seq_near = [seq_id(OWN, 1), seq_id(A), seq_id(B), seq_id(C)]
    ten_near = [ten_id(0, 1), ten_id(0, 3), ten_id(1, 0), ten_id(1, 1), ten_id(1, 3)]
    ten_all = [ten_id(0, 1), ten_id(0, 3), ten_id(0, 2), ten_id(1, 0), ten_id(1, 1), ten_id(1, 3)]
    own_rows = pl.ds(pl.multiple_of(ti * 192, 16), 192)
    loads = [
        pltpu.make_async_copy(w_out, wf.at[own_rows], lsem.at[0]),
        pltpu.make_async_copy(w_up, wu, lsem.at[1]),
        pltpu.make_async_copy(w_down, wd, lsem.at[2]),
        pltpu.make_async_copy(tokens, tok.at[0:ROWS], lsem.at[3]),
    ]
    for c in loads:
        c.start()
    barrier = pltpu.get_barrier_semaphore()
    for d in seq_near:
        pl.semaphore_signal(barrier, inc=1, device_id={"seq": d}, device_id_type=MESH)
    for d in ten_all:
        pl.semaphore_signal(barrier, inc=1, device_id={"tensor": d}, device_id_type=MESH)

    lane = lax.broadcasted_iota(jnp.int32, (16, PAD), 1)
    row = lax.broadcasted_iota(jnp.int32, (16, PAD), 0)
    ones = jnp.where((row == 0) & (lane < ROWS), 1.0, 0.0).astype(bf16)

    def fill(s, _):
        for h in range(4):
            vt[s, h, HD:64, :] = ones
        return 0

    lax.fori_loop(0, NSEQ, fill, 0)
    for h in range(4):
        kt[me, h] = qkv[1, h]
        vt[me, h, 0:HD, :] = qkv[2, h]
    peak[...] = jnp.full(peak.shape, -1e30, f32)
    acc[...] = jnp.zeros(acc.shape, f32)
    p0[ROWS:PAD, :] = jnp.zeros((PAD - ROWS, PAD), bf16)
    p1[ROWS:PAD, :] = jnp.zeros((PAD - ROWS, PAD), bf16)
    tok[ROWS:PAD, :] = jnp.zeros((PAD - ROWS, 1536), bf16)
    pl.semaphore_wait(barrier, len(seq_near) + len(ten_all))

    sent = [[], []]

    def block_ref(piece, slot, hp):
        ref = kt if piece == 0 else vt
        return ref.at[slot, 2 * hp : 2 * hp + 2, 0:HD]

    def seq_copy(piece, slot, hp, dest, index, own=False):
        src = qkv.at[1 + piece, 2 * hp : 2 * hp + 2] if own else block_ref(piece, slot, hp)
        return pltpu.make_async_remote_copy(
            src_ref=src, dst_ref=block_ref(piece, slot, hp), send_sem=ssem.at[hp, index],
            recv_sem=rsem.at[slot, hp, piece], device_id={"seq": dest}, device_id_type=MESH,
        )

    def send(piece, slot, hp, dest, own=False):
        c = seq_copy(piece, slot, hp, dest, len(sent[hp]), own)
        c.start()
        sent[hp].append(piece)

    def send_own(hp):
        for piece in (0, 1):
            for d in (seq_id(B), seq_id(A), seq_id(C), seq_id(OWN, 1)):
                send(piece, me, hp, d, own=True)

    def arrive(hp, off, other):
        slot = seq_id(off, other)
        for piece in (0, 1):
            seq_copy(piece, slot, hp, me, 0).wait_recv()
        if other:
            return
        if off in (A, D):
            send(0, slot, hp, seq_id(B))
        if off in (B, E):
            send(1, slot, hp, seq_id(A))
        for piece in (0, 1):
            send(piece, slot, hp, seq_id(OWN, 1))

    def spread(hp):
        slot = seq_id(C)
        for piece in (0, 1):
            for d in (seq_id(B), seq_id(A)):
                send(piece, slot, hp, d)

    tsent = []

    def head_ref(src, head):
        return att.at[pl.ds(pl.multiple_of(src * 192 + head * HD, 16), HD)]

    def ten_copy(src, head, dest, index):
        return pltpu.make_async_remote_copy(
            src_ref=head_ref(src, head), dst_ref=head_ref(src, head), send_sem=tsend.at[index],
            recv_sem=trecv.at[src, head], device_id={"tensor": dest}, device_id_type=MESH,
        )

    def ten_start(src, head, dest):
        c = ten_copy(src, head, dest, len(tsent))
        c.start()
        tsent.append(0)

    def finish(hp):
        for h in (2 * hp, 2 * hp + 1):
            att[pl.ds(pl.multiple_of(ti * 192 + h * HD, 16), HD), :] = (acc[h, 0:HD, :] / acc[h, HD : HD + 1, :]).astype(bf16)
        for h in (2 * hp, 2 * hp + 1):
            for d in ten_near:
                ten_start(ti, h, d)

    def ten_wait(src, head):
        ten_copy(src, head, ti, 0).wait_recv()

    def relay(hp):
        for dz in (0, 1):
            left, right = ten_id(dz, 3), ten_id(dz, 1)
            for h in (2 * hp, 2 * hp + 1):
                ten_wait(left, h)
                ten_wait(right, h)
            ten_start(left, 2 * hp, ten_id(0, 1))
            ten_start(right, 2 * hp + 1, ten_id(0, 3))

    def collect(hp):
        for h in (2 * hp, 2 * hp + 1):
            ten_wait(ten_id(1, 0), h)
            ten_wait(ten_id(0, 2), h)
            ten_wait(ten_id(1, 2), h)

    wsent = []

    def w_copy(src, half, other, dest, index):
        at = lax.rem(core + other, 2)
        ref = wf.at[pl.ds(pl.multiple_of(src * 192 + at * 96 + half * 48, 16), 48)]
        return pltpu.make_async_remote_copy(
            src_ref=ref, dst_ref=ref, send_sem=wsend.at[index], recv_sem=wrecv.at[src, other, half],
            device_id=dest, device_id_type=MESH,
        )

    def w_start(src, half, dest, index_other=0):
        at = core
        ref = wf.at[pl.ds(pl.multiple_of(src * 192 + at * 96 + half * 48, 16), 48)]
        pltpu.make_async_remote_copy(
            src_ref=ref, dst_ref=ref, send_sem=wsend.at[len(wsent)], recv_sem=wrecv.at[src, index_other, half],
            device_id=dest, device_id_type=MESH,
        ).start()
        wsent.append(0)

    def w_wait(src, half, other):
        w_copy(src, half, other, {"tensor": ti}, 0).wait_recv()

    def w_share(src):
        for half in (0, 1):
            w_start(src, half, {"seq": seq_id(OWN, 1)}, 1)

    def w_own():
        loads[0].wait()
        for half in (0, 1):
            for d in (ten_id(0, 1), ten_id(0, 3), ten_id(1, 0)):
                w_start(ti, half, {"tensor": d})

    def w_relay(dz):
        left, right = ten_id(dz, 3), ten_id(dz, 1)
        for src in (left, right):
            for half in (0, 1):
                w_wait(src, half, 0)
        w_start(left, 0, {"tensor": ten_id(0, 1)})
        w_start(right, 1, {"tensor": ten_id(0, 3)})
        w_share(left)
        w_share(right)

    def w_cross():
        src = ten_id(1, 0)
        for half in (0, 1):
            w_wait(src, half, 0)
            for d in (ten_id(0, 1), ten_id(0, 3)):
                w_start(src, half, {"tensor": d})
        w_share(src)

    def w_far(dz):
        src = ten_id(dz, 2)
        for half in (0, 1):
            w_wait(src, half, 0)
        w_share(src)

    def w_collect():
        for dz in (0, 1):
            for dx in range(4):
                if (dz, dx) != (0, 0):
                    for half in (0, 1):
                        w_wait(ten_id(dz, dx), half, 1)

    S, Pw = (s0, s1), (p0, p1)

    def slot_at(pos):
        code = pos * 0
        for j, (off, other) in enumerate(ORDER):
            code = code + (pos == j).astype(jnp.int32) * (DZ[off] * 8 + DY[off] * 2 + other)
        dz, dy, dc = lax.div(code, 8), lax.rem(lax.div(code, 2), 4), lax.rem(code, 2)
        return (lax.rem(zh + dz, 2) * 4 + lax.rem(yy + dy, 4)) * 2 + lax.rem(core + dc, 2)

    def score_pieces(slot, head, par, top):
        def mk(c, half):
            cs = slice(c * W, (c + 1) * W)

            def go():
                lo = half * 384
                n = 384 if half == 0 else ROWS - 384
                s = lax.dot_general(
                    kt[slot, head, :, lo : lo + 384], qkv[0, head, :, cs], (((0,), (0,)), ((), ())), preferred_element_type=f32
                )[0:n]
                S[par][lo : lo + n, cs] = s
                b = jnp.max(s.reshape(-1, 8, W), axis=0)
                top[c] = b if c not in top else jnp.maximum(top[c], b)

            return go

        return [mk(c, half) for c in range(NC) for half in (0, 1)]

    def weight_pieces(par, now):
        def mk(c, r):
            cs = slice(c * W, (c + 1) * W)

            def go():
                Pw[par][r : r + 240, cs] = jnp.exp2(S[par][r : r + 240, cs] - now[c]).astype(bf16)

            return go

        return [mk(c, r) for c in range(NC) for r in (0, 240, 480)]

    def value_pieces(slot, head, par, factor):
        def mk(c):
            cs = slice(c * W, (c + 1) * W)

            def go():
                acc[head, :, cs] = acc[head, :, cs] * factor[c] + jnp.dot(
                    vt[slot, head], Pw[par][:, cs], preferred_element_type=f32
                )

            return go

        return [mk(c) for c in range(NC)]

    def interleave(*lists):
        events = []
        for k, items in enumerate(lists):
            for j, x in enumerate(items):
                events.append(((j + 0.5) / len(items), k, x))
        events.sort(key=lambda e: (e[0], e[1]))
        for _, _, x in events:
            x()

    def keep_top(head, top):
        for c in range(NC):
            peak[head, 8:16, c * W : (c + 1) * W] = top[c]

    def step(t, _):
        for hp in (0, 1):
            for j, blocks in ARRIVE.items():

                @pl.when(t == 16 * hp + j)
                def _(hp=hp, j=j, blocks=blocks):
                    for off, other in blocks:
                        arrive(hp, off, other)
                    if j == 1:
                        spread(hp)
                    if j == 9 and hp == 0:
                        send_own(1)

        @pl.when(t == 5)
        def _():
            w_cross()
            w_relay(0)

        @pl.when(t == 12)
        def _():
            w_relay(1)
            w_far(0)

        @pl.when(t == 15)
        def _():
            w_far(1)

        @pl.when(t == 16)
        def _():
            finish(0)

        @pl.when(t == 22)
        def _():
            relay(0)

        @pl.when(t == 28)
        def _():
            collect(0)
            w_collect()

        hp = lax.div(t, 16)
        slot = slot_at(lax.rem(t, 16))
        nxt = lax.rem(t + 1, 32)
        slot_next = slot_at(lax.rem(nxt, 16))
        held = None
        for k in (0, 1):
            head = 2 * hp + k
            now, factor = {}, {}
            for c in range(NC):
                cs = slice(c * W, (c + 1) * W)
                old = peak[head, 0:1, cs]
                now[c] = jnp.maximum(old, jnp.max(peak[head, 8:16, cs], axis=0, keepdims=True))
                factor[c] = jnp.exp2(old - now[c])
                peak[head, 0:1, cs] = now[c]
            head_n = head + 1 if k == 0 else 2 * lax.div(nxt, 16)
            slot_n = slot if k == 0 else slot_next
            top = {}
            scores = score_pieces(slot_n, head_n, 1 - k, top)
            weights = weight_pieces(k, now)
            if held is None:
                interleave(scores, weights)
                held = value_pieces(slot, head, k, factor)
            else:
                interleave(scores, weights, held)
                for x in value_pieces(slot, head, k, factor):
                    x()
            keep_top(head_n, top)
        return 0

    send_own(0)
    w_own()
    top = {}
    for x in score_pieces(me, 0, 0, top):
        x()
    keep_top(0, top)
    lax.fori_loop(0, 32, step, 0)
    finish(1)
    relay(1)
    collect(1)
    for c in loads[1:]:
        c.wait()

    def project(c, _):
        cols = pl.ds(pl.multiple_of(c * W, W), W)
        m = tok[cols, :].astype(f32) + lax.dot_general(
            att[:, cols], wf[...], (((0,), (0,)), ((), ())), preferred_element_type=f32
        )
        mixed[cols, :] = m
        post[cols, :] = layer_norm(m, gain[...]).astype(bf16)
        return 0

    lax.fori_loop(0, NC, project, 0)

    def rows_of(t, half=0, n=48):
        return pl.ds(pl.multiple_of(t * 96 + half * 48, 16), n)

    qsent = []

    def q_copy(src_ref, dst_ref, recv, dest, index):
        return pltpu.make_async_remote_copy(
            src_ref=src_ref, dst_ref=dst_ref, send_sem=qsend.at[index], recv_sem=recv,
            device_id={"tensor": dest}, device_id_type=MESH,
        )

    def q_start(src_ref, dst_ref, recv, dest):
        q_copy(src_ref, dst_ref, recv, dest, len(qsent)).start()
        qsent.append(0)

    def q_wait(ref, recv):
        q_copy(ref, ref, recv, ti, 0).wait_recv()

    def part(t, half):
        return term[rows_of(t, half), :].astype(f32)

    for dx in (2, 1, 3, 0):
        t0, t1 = ten_id(0, dx), ten_id(1, dx)
        both = jnp.concatenate([post[rows_of(t0, 0, 96), :], post[rows_of(t1, 0, 96), :]], axis=0)
        u = jnp.dot(both, wu[...], preferred_element_type=f32)
        h = jax.nn.gelu(u, approximate=True).astype(bf16)
        y = jnp.dot(h, wd[...], preferred_element_type=f32).astype(bf16)
        term[rows_of(t0, 0, 96), :] = y[0:96]
        term[rows_of(t1, 0, 96), :] = y[96:192]
        q_start(term.at[rows_of(t1, 1)], rb.at[dx], rbrecv.at[dx], ten_id(1, 0))
        if dx:
            for dz, t in ((1, t1), (0, t0)):
                q_start(term.at[rows_of(t, 0)], ra.at[dz, 3 - dx], rarecv.at[dz, 3 - dx], t0)
    for dx in (2, 1, 3):
        q_wait(rb.at[dx], rbrecv.at[dx])
        sb2[dx - 1] = (part(ten_id(0, dx), 1) + rb[dx].astype(f32)).astype(bf16)
        q_start(sb2.at[dx - 1], rb2.at[3 - dx], rb2recv.at[3 - dx], ten_id(0, dx))
    total = part(ten_id(1, 0), 0)
    for k in range(3):
        q_wait(ra.at[1, k], rarecv.at[1, k])
        total = total + ra[1, k].astype(f32)
    sa2[...] = total.astype(bf16)
    q_start(sa2, ra2, ra2recv.at[0], ten_id(1, 0))

    gsent = []

    def g_copy(t, half, dest, index):
        ref = out.at[rows_of(t, half)]
        return pltpu.make_async_remote_copy(
            src_ref=ref, dst_ref=ref, send_sem=gsend.at[index], recv_sem=grecv.at[t, half],
            device_id={"tensor": dest}, device_id_type=MESH,
        )

    def g_start(t, half, dest):
        g_copy(t, half, dest, len(gsent)).start()
        gsent.append(0)

    def g_wait(t, half):
        g_copy(t, half, ti, 0).wait_recv()

    q_wait(rb.at[0], rbrecv.at[0])
    total = mixed[rows_of(ti, 1), :] + part(ti, 1) + rb[0].astype(f32)
    for k in range(3):
        q_wait(rb2.at[k], rb2recv.at[k])
        total = total + rb2[k].astype(f32)
    out[rows_of(ti, 1), :] = total.astype(bf16)
    g_start(ti, 1, ten_id(1, 0))
    total = mixed[rows_of(ti, 0), :] + part(ti, 0)
    for k in range(3):
        q_wait(ra.at[0, k], rarecv.at[0, k])
        total = total + ra[0, k].astype(f32)
    q_wait(ra2, ra2recv.at[0])
    total = total + ra2[...].astype(f32)
    out[rows_of(ti, 0), :] = total.astype(bf16)
    for dx in (1, 3, 2):
        g_start(ti, 0, ten_id(0, dx))
    g_start(ti, 0, ten_id(1, 0))
    for dx in (1, 3, 2):
        g_start(ti, 1, ten_id(0, dx))
    g_wait(ten_id(1, 0), 1)
    for dx in (1, 3, 2):
        g_start(ten_id(1, 0), 1, ten_id(0, dx))
    for dx in (1, 3, 2):
        g_wait(ten_id(0, dx), 0)
        g_start(ten_id(0, dx), 0, ten_id(1, 0))
    for dx in (1, 3, 2):
        g_wait(ten_id(0, dx), 1)
    g_wait(ten_id(1, 0), 0)
    for dx in (1, 3, 2):
        g_wait(ten_id(1, dx), 0)
        g_wait(ten_id(1, dx), 1)

    for hp in (0, 1):
        for index, piece in enumerate(sent[hp]):
            seq_copy(piece, me, hp, me, index).wait_send()
    for index in range(len(tsent)):
        ten_copy(ti, 0, ti, index).wait_send()
    for index in range(len(wsent)):
        w_copy(ti, 0, 0, {"tensor": ti}, index).wait_send()
    for index in range(len(qsent)):
        q_copy(sa2, ra2, ra2recv.at[0], ti, index).wait_send()
    for index in range(len(gsent)):
        g_copy(ti, 0, ti, index).wait_send()


def layer(qkv, gain, tokens, w_out, w_up, w_down):
    vmem = pl.BlockSpec(memory_space=pltpu.VMEM)
    hbm = pl.BlockSpec(memory_space=pl.ANY)
    D = tokens.shape[1]
    return pl.pallas_call(
        layer_kernel,
        out_shape=jax.ShapeDtypeStruct((PAD, D), bf16),
        in_specs=[vmem, vmem, hbm, hbm, hbm, hbm],
        out_specs=vmem,
        scratch_shapes=[
            pltpu.VMEM((NSEQ, 4, HD, PAD), bf16),
            pltpu.VMEM((NSEQ, 4, 64, PAD), bf16),
            pltpu.VMEM((ROWS, PAD), f32),
            pltpu.VMEM((ROWS, PAD), f32),
            pltpu.VMEM((PAD, PAD), bf16),
            pltpu.VMEM((PAD, PAD), bf16),
            pltpu.VMEM((4, 64, PAD), f32),
            pltpu.VMEM((4, 16, PAD), f32),
            pltpu.VMEM((D, PAD), bf16),
            pltpu.VMEM((D, D), bf16),
            pltpu.VMEM((PAD, D), bf16),
            pltpu.VMEM((D, 768), bf16),
            pltpu.VMEM((768, D), bf16),
            pltpu.VMEM((PAD, D), f32),
            pltpu.VMEM((PAD, D), bf16),
            pltpu.VMEM((PAD, D), bf16),
            pltpu.VMEM((2, 3, 48, D), bf16),
            pltpu.VMEM((4, 48, D), bf16),
            pltpu.VMEM((48, D), bf16),
            pltpu.VMEM((3, 48, D), bf16),
            pltpu.VMEM((48, D), bf16),
            pltpu.VMEM((3, 48, D), bf16),
            pltpu.SemaphoreType.DMA((2, 32)),
            pltpu.SemaphoreType.DMA((NSEQ, 2, 2)),
            pltpu.SemaphoreType.DMA((32,)),
            pltpu.SemaphoreType.DMA((NTEN, 4)),
            pltpu.SemaphoreType.DMA((32,)),
            pltpu.SemaphoreType.DMA((NTEN, 2, 2)),
            pltpu.SemaphoreType.DMA((4,)),
            pltpu.SemaphoreType.DMA((16,)),
            pltpu.SemaphoreType.DMA((2, 3)),
            pltpu.SemaphoreType.DMA((4,)),
            pltpu.SemaphoreType.DMA((1,)),
            pltpu.SemaphoreType.DMA((3,)),
            pltpu.SemaphoreType.DMA((16,)),
            pltpu.SemaphoreType.DMA((NTEN, 2)),
        ],
        compiler_params=pltpu.CompilerParams(collective_id=0, has_side_effects=True, vmem_limit_bytes=60 * 2**20),
        cost_estimate=pl.CostEstimate(flops=60_000_000_000, bytes_accessed=4_000_000, transcendentals=33_000_000),
        name="layer",
    )(qkv, gain, tokens, w_out, w_up, w_down)


def per_device(tokens, norm_gain, w_qkv, w_out, post_gain, w_up, w_down):
    base = tokens.astype(f32)
    normed = layer_norm(base, norm_gain).astype(bf16)
    qkv = lax.dot_general(w_qkv.reshape(w_qkv.shape[0], -1), normed, (((0,), (1,)), ((), ())), preferred_element_type=f32)
    scale = jnp.concatenate([jnp.full((192, 1), 1.4426950408889634 / HD**0.5, f32), jnp.ones((384, 1), f32)])
    qkv = jnp.pad((qkv * scale).astype(bf16), ((0, 0), (0, PAD - ROWS))).reshape(3, 4, HD, PAD)
    return layer(qkv, post_gain[None, :], tokens, w_out, w_up, w_down)[:ROWS]


def solution(mesh):
    placed = (P("seq", None), P(), P(None, None, "tensor"), P("tensor", None), P(), P(None, "tensor"), P("tensor", None))
    return jax.shard_map(per_device, mesh=mesh, in_specs=placed, out_specs=P("seq", None), check_vma=False)
```

```python
import functools

import jax
import jax.numpy as jnp
from jax import lax
from jax.experimental import pallas as pl
from jax.experimental.pallas import tpu as pltpu
from jax.sharding import PartitionSpec as P

HD = 48
ROWS = 720
PAD = 768
NSEQ = 16
NTEN = 8
W = 256
NC = PAD // W
f32 = jnp.float32
bf16 = jnp.bfloat16
MESH = pl.DeviceIdType.MESH

OWN, A, B, C, F, D, E, G = range(8)
DZ = (0, 0, 0, 1, 0, 1, 1, 1)
DY = (0, 3, 1, 0, 2, 3, 1, 2)
ARRIVE = {
    0: ((0, OWN, 1),), 1: ((0, A, 0), (0, B, 0), (0, C, 0)), 4: ((0, A, 1),), 5: ((0, B, 1),), 6: ((0, C, 1), (0, D, 0), (0, E, 0)),
       9: ((0, D, 1),), 10: ((0, E, 1),), 11: ((0, F, 0),), 12: ((0, G, 0),), 13: ((0, F, 1),),
    14: ((0, G, 1),), 15: ((1, OWN, 1),), 16: ((1, A, 0), (1, B, 0), (1, C, 0)), 20: ((1, A, 1),), 21: ((1, B, 1), (1, D, 0), (1, E, 0)),
    22: ((1, C, 1),), 23: ((1, D, 1),), 24: ((1, E, 1), (1, F, 0)), 25: ((1, G, 0), (1, F, 1)), 26: ((1, G, 1),),
}


def layer_norm(values, gain):
    mean = jnp.mean(values, axis=-1, keepdims=True)
    centred = values - mean
    var = jnp.mean(centred * centred, axis=-1, keepdims=True)
    return centred * lax.rsqrt(var + 1e-05) * gain


def layer_kernel(qkv, gain, tokens, w_out, w_up, w_down, out, kt, vt, s0, s1, p0, p1, acc, peak, att, wf, tok, wu, wd,
                 mixed, post, term, ra, rb, ra2, rb2, sa2, sb2, ssem, rsem, tsend, trecv, wsend, wrecv, lsem,
                 qsend, rarecv, rbrecv, ra2recv, rb2recv, gsend, grecv):
    me = lax.axis_index("seq")
    ti = lax.axis_index("tensor")
    zh, yy, core = lax.div(me, 8), lax.rem(lax.div(me, 2), 4), lax.rem(me, 2)
    zl, xx = lax.div(ti, 4), lax.rem(ti, 4)

    def seq_id(off, other=0):
        return (lax.rem(zh + DZ[off], 2) * 4 + lax.rem(yy + DY[off], 4)) * 2 + lax.rem(core + other, 2)

    def ten_id(dz, dx):
        return lax.rem(zl + dz, 2) * 4 + lax.rem(xx + dx, 4)

    seq_near = [seq_id(OWN, 1), seq_id(A), seq_id(B), seq_id(C)]
    ten_near = [ten_id(0, 1), ten_id(0, 3), ten_id(1, 0), ten_id(1, 1), ten_id(1, 3)]
    ten_all = [ten_id(0, 1), ten_id(0, 3), ten_id(0, 2), ten_id(1, 0), ten_id(1, 1), ten_id(1, 3)]
    loads = [
        pltpu.make_async_copy(w_up, wu, lsem.at[0]),
        pltpu.make_async_copy(w_down, wd, lsem.at[1]),
        pltpu.make_async_copy(tokens, tok.at[0:ROWS], lsem.at[2]),
    ]
    loads += [
        pltpu.make_async_copy(
            w_out.at[h * HD : (h + 1) * HD], wf.at[pl.ds(pl.multiple_of(h * 384 + ti * HD, 16), HD)], lsem.at[3 + h]
        )
        for h in range(4)
    ]
    for c in loads:
        c.start()
    barrier = pltpu.get_barrier_semaphore()
    for d in seq_near:
        pl.semaphore_signal(barrier, inc=1, device_id={"seq": d}, device_id_type=MESH)
    for d in ten_all:
        pl.semaphore_signal(barrier, inc=1, device_id={"tensor": d}, device_id_type=MESH)

    lane = lax.broadcasted_iota(jnp.int32, (16, PAD), 1)
    row = lax.broadcasted_iota(jnp.int32, (16, PAD), 0)
    ones = jnp.where((row == 0) & (lane < ROWS), 1.0, 0.0).astype(bf16)

    def fill(s, _):
        for h in range(4):
            vt[s, h, HD:64, :] = ones
        return 0

    lax.fori_loop(0, NSEQ, fill, 0)
    for h in range(4):
        kt[me, h] = qkv[1, h]
        vt[me, h, 0:HD, :] = qkv[2, h]
    peak[0:4] = jnp.full((4, 16, PAD), -1e30, f32)
    peak[4:6] = jnp.ones((2, 16, PAD), f32)
    acc[...] = jnp.zeros(acc.shape, f32)
    p0[ROWS:PAD, :] = jnp.zeros((PAD - ROWS, PAD), bf16)
    p1[...] = jnp.zeros((PAD, PAD), bf16)
    tok[ROWS:PAD, :] = jnp.zeros((PAD - ROWS, 1536), bf16)
    pl.semaphore_wait(barrier, len(seq_near) + len(ten_all))

    sent = [[], []]

    def block_ref(piece, slot, hp):
        ref = kt if piece == 0 else vt
        return ref.at[slot, 2 * hp : 2 * hp + 2, 0:HD]

    def seq_copy(piece, slot, hp, dest, index, own=False):
        src = qkv.at[1 + piece, 2 * hp : 2 * hp + 2] if own else block_ref(piece, slot, hp)
        return pltpu.make_async_remote_copy(
            src_ref=src, dst_ref=block_ref(piece, slot, hp), send_sem=ssem.at[hp, index],
            recv_sem=rsem.at[slot, hp, piece], device_id={"seq": dest}, device_id_type=MESH,
        )

    def send(piece, slot, hp, dest, own=False):
        c = seq_copy(piece, slot, hp, dest, len(sent[hp]), own)
        c.start()
        sent[hp].append(piece)

    def send_own(hp):
        for piece in (0, 1):
            for d in (seq_id(B), seq_id(A), seq_id(C), seq_id(OWN, 1)):
                send(piece, me, hp, d, own=True)

    def arrive(hp, off, other):
        slot = seq_id(off, other)
        for piece in (0, 1):
            seq_copy(piece, slot, hp, me, 0).wait_recv()
        if other:
            return
        if off in (D, E):
            onward(hp, off)
        for piece in (0, 1):
            send(piece, slot, hp, seq_id(OWN, 1))

    def onward(hp, off):
        if off in (A, D):
            send(0, seq_id(off), hp, seq_id(B))
        else:
            send(1, seq_id(off), hp, seq_id(A))

    def spread(hp):
        slot = seq_id(C)
        for piece in (0, 1):
            for d in (seq_id(B), seq_id(A)):
                send(piece, slot, hp, d)
        onward(hp, A)
        onward(hp, B)

    tsent = []

    def head_ref(src, head):
        return att.at[pl.ds(pl.multiple_of(head * 384 + src * HD, 16), HD)]

    def ten_copy(src, head, dest, index):
        return pltpu.make_async_remote_copy(
            src_ref=head_ref(src, head), dst_ref=head_ref(src, head), send_sem=tsend.at[index],
            recv_sem=trecv.at[src, head], device_id={"tensor": dest}, device_id_type=MESH,
        )

    def ten_start(src, head, dest):
        c = ten_copy(src, head, dest, len(tsent))
        c.start()
        tsent.append(0)

    def finish(heads):
        for h in heads:
            att[pl.ds(pl.multiple_of(h * 384 + ti * HD, 16), HD), :] = (acc[h, 0:HD, :] / acc[h, HD : HD + 1, :]).astype(bf16)
        for h in heads:
            for d in ten_near:
                ten_start(ti, h, d)

    def ten_wait(src, head):
        ten_copy(src, head, ti, 0).wait_recv()

    def relay(head):
        for src, dest in ((ten_id(0, 3), ten_id(0, 1)), (ten_id(1, 1), ten_id(0, 3))):
            ten_wait(src, head)
            ten_start(src, head, dest)

    def collect(head):
        for src in (ten_id(0, 1), ten_id(1, 3), ten_id(1, 0), ten_id(0, 2), ten_id(1, 2)):
            ten_wait(src, head)

    wsent = []

    def w_copy(src, half, other, dest, index):
        at = lax.rem(core + other, 2)
        ref = wf.at[pl.ds(pl.multiple_of((at * 2 + half) * 384 + src * HD, 16), HD)]
        return pltpu.make_async_remote_copy(
            src_ref=ref, dst_ref=ref, send_sem=wsend.at[index], recv_sem=wrecv.at[src, other, half],
            device_id=dest, device_id_type=MESH,
        )

    def w_start(src, half, dest, index_other=0):
        at = core
        ref = wf.at[pl.ds(pl.multiple_of((at * 2 + half) * 384 + src * HD, 16), HD)]
        pltpu.make_async_remote_copy(
            src_ref=ref, dst_ref=ref, send_sem=wsend.at[len(wsent)], recv_sem=wrecv.at[src, index_other, half],
            device_id=dest, device_id_type=MESH,
        ).start()
        wsent.append(0)

    def w_wait(src, half, other):
        w_copy(src, half, other, {"tensor": ti}, 0).wait_recv()

    def w_share(src):
        for half in (0, 1):
            w_start(src, half, {"seq": seq_id(OWN, 1)}, 1)

    def w_own():
        for c in loads[3:]:
            c.wait()
        for half in (0, 1):
            for d in (ten_id(0, 1), ten_id(0, 3), ten_id(1, 0)):
                w_start(ti, half, {"tensor": d})

    def w_relay(dz):
        left, right = ten_id(dz, 3), ten_id(dz, 1)
        for src in (left, right):
            for half in (0, 1):
                w_wait(src, half, 0)
        w_start(left, 0, {"tensor": ten_id(0, 1)})
        w_start(right, 1, {"tensor": ten_id(0, 3)})
        w_share(left)
        w_share(right)

    def w_cross():
        src = ten_id(1, 0)
        for half in (0, 1):
            w_wait(src, half, 0)
            for d in (ten_id(0, 1), ten_id(0, 3)):
                w_start(src, half, {"tensor": d})
        w_share(src)

    def w_far(dz):
        src = ten_id(dz, 2)
        for half in (0, 1):
            w_wait(src, half, 0)
        w_share(src)

    def w_collect():
        for dz in (0, 1):
            for dx in range(4):
                if (dz, dx) != (0, 0):
                    for half in (0, 1):
                        w_wait(ten_id(dz, dx), half, 1)

    S, Pw = (s0, s1), (p0, p1)

    def slot_at(pos):
        mid, late = (pos >= 2).astype(jnp.int32), (pos >= 8).astype(jnp.int32)
        q, r = lax.rem(pos + 4, 6), lax.rem(pos, 4)
        chip = mid * (1 - late) * (1 + lax.rem(q, 3)) + late * (2 * lax.div(pos, 4) + lax.rem(r, 2))
        other = (1 - mid) * pos + mid * (1 - late) * lax.div(q, 3) + late * lax.div(r, 2)
        far = (chip >= 6).astype(jnp.int32)
        dy = (1 - far) * lax.rem(3 * lax.rem(chip, 3), 5) + 2 * far
        dz = (1 - far) * lax.div(chip, 3) + far * (chip - 6)
        return (lax.rem(zh + dz, 2) * 4 + lax.rem(yy + dy, 4)) * 2 + lax.rem(core + other, 2)

    def score_pieces(slot, head, par, top):
        def mk(c, half):
            cs = slice(c * W, (c + 1) * W)

            def go():
                lo = half * 384
                n = 384 if half == 0 else ROWS - 384
                s = lax.dot_general(
                    kt[slot, head, :, lo : lo + 384], qkv[0, head, :, cs], (((0,), (0,)), ((), ())), preferred_element_type=f32
                )[0:n]
                S[par][lo : lo + n, cs] = s
                b = jnp.max(s.reshape(-1, 8, W), axis=0)
                top[c] = b if c not in top else jnp.maximum(top[c], b)

            return go

        return [mk(c, half) for c in range(NC) for half in (0, 1)]

    def weight_pieces(par, now):
        def mk(c, r):
            cs = slice(c * W, (c + 1) * W)

            def go():
                Pw[par][r : r + 240, cs] = jnp.exp2(S[par][r : r + 240, cs] - now[c]).astype(bf16)

            return go

        return [mk(c, r) for c in range(NC) for r in (0, 240, 480)]

    def value_pieces(slot, head, par, factor):
        def mk(c):
            cs = slice(c * W, (c + 1) * W)

            def go():
                acc[head, :, cs] = acc[head, :, cs] * factor[c] + jnp.dot(
                    vt[slot, head], Pw[par][:, cs], preferred_element_type=f32
                )

            return go

        return [mk(c) for c in range(NC)]

    def interleave(*lists):
        events = []
        for k, items in enumerate(lists):
            for j, x in enumerate(items):
                events.append(((j + 0.5) / len(items), k, x))
        events.sort(key=lambda e: (e[0], e[1]))
        for _, _, x in events:
            x()

    def keep_top(head, top):
        for c in range(NC):
            peak[head, 8:16, c * W : (c + 1) * W] = top[c]

    def item(n):
        n = lax.rem(n, 64)
        late = (n >= 44).astype(jnp.int32)
        last = (n >= 54).astype(jnp.int32)
        pos = (1 - late) * lax.div(lax.rem(n, 32), 2) + late * (n - 38 - 10 * last)
        head = (1 - late) * (2 * lax.div(n, 32) + lax.rem(n, 2)) + late * (2 + last)
        return slot_at(pos), head

    def step(t, held):
        def events(at):
            for hp, off, other in ARRIVE.get(at, ()):
                arrive(hp, off, other)
            if at == 1:
                spread(0)
            if at == 5:
                w_cross()
                w_relay(0)
            if at == 7:
                send_own(1)
            if at == 12:
                w_relay(1)
                w_far(0)
            if at == 15:
                w_far(1)
            if at == 16:
                spread(1)
            if at == 17:
                finish((0, 1))
            if at == 24:
                relay(0)
                relay(1)
            if at == 30:
                collect(0)
                collect(1)
                w_collect()
            if at == 28:
                finish((2,))

        at_all = sorted(set(ARRIVE) | {1, 5, 7, 12, 15, 16, 17, 24, 28, 30})

        def search(lo, hi):
            inside = [at for at in at_all if lo <= at < hi]
            if not inside:
                return
            if hi - lo == 1:
                events(lo)
                return
            mid = (lo + hi) // 2
            for a, b in ((lo, mid), (mid, hi)):
                if any(a <= at < b for at in inside):
                    test = t < mid if a == lo else t >= mid
                    pl.when(test)(functools.partial(search, a, b))

        search(0, 32)
        slots = {q: item(2 * t + q) for q in (1, 2)}
        slots[-1], slots[0] = (held[0], held[1]), (held[2], held[3])
        for k in (0, 1):
            (slot_p, head_p), (slot, head), (slot_n, head_n) = slots[k - 1], slots[k], slots[k + 1]
            now, factor_p = {}, {}
            for c in range(NC):
                cs = slice(c * W, (c + 1) * W)
                factor_p[c] = peak[5 - k, 0:1, cs]
                old = peak[head, 0:1, cs]
                now[c] = jnp.maximum(old, jnp.max(peak[head, 8:16, cs], axis=0, keepdims=True))
                peak[4 + k, 0:1, cs] = jnp.exp2(old - now[c])
                peak[head, 0:1, cs] = now[c]
            top = {}
            interleave(
                score_pieces(slot_n, head_n, 1 - k, top),
                weight_pieces(k, now),
                value_pieces(slot_p, head_p, 1 - k, factor_p),
            )
            keep_top(head_n, top)
        return (*slots[1], *slots[2])

    send_own(0)
    w_own()
    top = {}
    for x in score_pieces(me, 0, 0, top):
        x()
    keep_top(0, top)
    lax.fori_loop(0, 32, step, (me, me * 0, me, me * 0))
    for x in value_pieces(slot_at(me * 0 + 15), 3, 1, {c: peak[5, 0:1, c * W : (c + 1) * W] for c in range(NC)}):
        x()
    finish((3,))
    relay(2)
    for c in loads[:3]:
        c.wait()

    def project(c, _):
        cols = pl.ds(pl.multiple_of(c * W, W), W)
        mixed[cols, :] = tok[cols, :].astype(f32) + lax.dot_general(
            att[0:768, cols], wf[0:768, :], (((0,), (0,)), ((), ())), preferred_element_type=f32
        )
        return 0

    lax.fori_loop(0, NC, project, 0)
    relay(3)
    collect(2)
    collect(3)

    def complete(c, _):
        cols = pl.ds(pl.multiple_of(c * W, W), W)
        m = mixed[cols, :] + lax.dot_general(
            att[768:1536, cols], wf[768:1536, :], (((0,), (0,)), ((), ())), preferred_element_type=f32
        )
        mixed[cols, :] = m
        post[cols, :] = layer_norm(m, gain[...]).astype(bf16)
        return 0

    lax.fori_loop(0, NC, complete, 0)

    def rows_of(t, half=0, n=48):
        return pl.ds(pl.multiple_of(t * 96 + half * 48, 16), n)

    qsent = []

    def q_copy(src_ref, dst_ref, recv, dest, index):
        return pltpu.make_async_remote_copy(
            src_ref=src_ref, dst_ref=dst_ref, send_sem=qsend.at[index], recv_sem=recv,
            device_id={"tensor": dest}, device_id_type=MESH,
        )

    def q_start(src_ref, dst_ref, recv, dest):
        q_copy(src_ref, dst_ref, recv, dest, len(qsent)).start()
        qsent.append(0)

    def q_wait(ref, recv):
        q_copy(ref, ref, recv, ti, 0).wait_recv()

    def part(t, half):
        return term[rows_of(t, half), :].astype(f32)

    for dx in (2, 1, 3, 0):
        t0, t1 = ten_id(0, dx), ten_id(1, dx)
        both = jnp.concatenate([post[rows_of(t0, 0, 96), :], post[rows_of(t1, 0, 96), :]], axis=0)
        u = jnp.dot(both, wu[...], preferred_element_type=f32)
        h = jax.nn.gelu(u, approximate=True).astype(bf16)
        y = jnp.dot(h, wd[...], preferred_element_type=f32).astype(bf16)
        term[rows_of(t0, 0, 96), :] = y[0:96]
        term[rows_of(t1, 0, 96), :] = y[96:192]
        q_start(term.at[rows_of(t1, 1)], rb.at[dx], rbrecv.at[dx], ten_id(1, 0))
        if dx:
            for dz, t in ((1, t1), (0, t0)):
                q_start(term.at[rows_of(t, 0)], ra.at[dz, 3 - dx], rarecv.at[dz, 3 - dx], t0)
    for dx in (2, 1, 3):
        q_wait(rb.at[dx], rbrecv.at[dx])
        sb2[dx - 1] = (part(ten_id(0, dx), 1) + rb[dx].astype(f32)).astype(bf16)
        q_start(sb2.at[dx - 1], rb2.at[3 - dx], rb2recv.at[3 - dx], ten_id(0, dx))
    total = part(ten_id(1, 0), 0)
    for k in range(3):
        q_wait(ra.at[1, k], rarecv.at[1, k])
        total = total + ra[1, k].astype(f32)
    sa2[...] = total.astype(bf16)
    q_start(sa2, ra2, ra2recv.at[0], ten_id(1, 0))

    gsent = []

    def g_copy(t, half, dest, index):
        ref = out.at[rows_of(t, half)]
        return pltpu.make_async_remote_copy(
            src_ref=ref, dst_ref=ref, send_sem=gsend.at[index], recv_sem=grecv.at[t, half],
            device_id={"tensor": dest}, device_id_type=MESH,
        )

    def g_start(t, half, dest):
        g_copy(t, half, dest, len(gsent)).start()
        gsent.append(0)

    def g_wait(t, half):
        g_copy(t, half, ti, 0).wait_recv()

    q_wait(rb.at[0], rbrecv.at[0])
    total = mixed[rows_of(ti, 1), :] + part(ti, 1) + rb[0].astype(f32)
    for k in range(3):
        q_wait(rb2.at[k], rb2recv.at[k])
        total = total + rb2[k].astype(f32)
    out[rows_of(ti, 1), :] = total.astype(bf16)
    g_start(ti, 1, ten_id(1, 0))
    total = mixed[rows_of(ti, 0), :] + part(ti, 0)
    for k in range(3):
        q_wait(ra.at[0, k], rarecv.at[0, k])
        total = total + ra[0, k].astype(f32)
    q_wait(ra2, ra2recv.at[0])
    total = total + ra2[...].astype(f32)
    out[rows_of(ti, 0), :] = total.astype(bf16)
    for dx in (1, 3, 2):
        g_start(ti, 0, ten_id(0, dx))
    g_start(ti, 0, ten_id(1, 0))
    for dx in (1, 3, 2):
        g_start(ti, 1, ten_id(0, dx))
    g_wait(ten_id(1, 0), 1)
    for dx in (1, 3, 2):
        g_start(ten_id(1, 0), 1, ten_id(0, dx))
    for dx in (1, 3, 2):
        g_wait(ten_id(0, dx), 0)
        g_start(ten_id(0, dx), 0, ten_id(1, 0))
    for dx in (1, 3, 2):
        g_wait(ten_id(0, dx), 1)
    g_wait(ten_id(1, 0), 0)
    for dx in (1, 3, 2):
        g_wait(ten_id(1, dx), 0)
        g_wait(ten_id(1, dx), 1)

    for hp in (0, 1):
        for index, piece in enumerate(sent[hp]):
            seq_copy(piece, me, hp, me, index).wait_send()
    for index in range(len(tsent)):
        ten_copy(ti, 0, ti, index).wait_send()
    for index in range(len(wsent)):
        w_copy(ti, 0, 0, {"tensor": ti}, index).wait_send()
    for index in range(len(qsent)):
        q_copy(sa2, ra2, ra2recv.at[0], ti, index).wait_send()
    for index in range(len(gsent)):
        g_copy(ti, 0, ti, index).wait_send()


def layer(qkv, gain, tokens, w_out, w_up, w_down):
    vmem = pl.BlockSpec(memory_space=pltpu.VMEM)
    hbm = pl.BlockSpec(memory_space=pl.ANY)
    D = tokens.shape[1]
    return pl.pallas_call(
        layer_kernel,
        out_shape=jax.ShapeDtypeStruct((PAD, D), bf16),
        in_specs=[vmem, vmem, hbm, hbm, hbm, hbm],
        out_specs=vmem,
        scratch_shapes=[
            pltpu.VMEM((NSEQ, 4, HD, PAD), bf16),
            pltpu.VMEM((NSEQ, 4, 64, PAD), bf16),
            pltpu.VMEM((ROWS, PAD), f32),
            pltpu.VMEM((ROWS, PAD), f32),
            pltpu.VMEM((PAD, PAD), bf16),
            pltpu.VMEM((PAD, PAD), bf16),
            pltpu.VMEM((4, 64, PAD), f32),
            pltpu.VMEM((6, 16, PAD), f32),
            pltpu.VMEM((D, PAD), bf16),
            pltpu.VMEM((D, D), bf16),
            pltpu.VMEM((PAD, D), bf16),
            pltpu.VMEM((D, 768), bf16),
            pltpu.VMEM((768, D), bf16),
            pltpu.VMEM((PAD, D), f32),
            pltpu.VMEM((PAD, D), bf16),
            pltpu.VMEM((PAD, D), bf16),
            pltpu.VMEM((2, 3, 48, D), bf16),
            pltpu.VMEM((4, 48, D), bf16),
            pltpu.VMEM((48, D), bf16),
            pltpu.VMEM((3, 48, D), bf16),
            pltpu.VMEM((48, D), bf16),
            pltpu.VMEM((3, 48, D), bf16),
            pltpu.SemaphoreType.DMA((2, 32)),
            pltpu.SemaphoreType.DMA((NSEQ, 2, 2)),
            pltpu.SemaphoreType.DMA((32,)),
            pltpu.SemaphoreType.DMA((NTEN, 4)),
            pltpu.SemaphoreType.DMA((32,)),
            pltpu.SemaphoreType.DMA((NTEN, 2, 2)),
            pltpu.SemaphoreType.DMA((7,)),
            pltpu.SemaphoreType.DMA((16,)),
            pltpu.SemaphoreType.DMA((2, 3)),
            pltpu.SemaphoreType.DMA((4,)),
            pltpu.SemaphoreType.DMA((1,)),
            pltpu.SemaphoreType.DMA((3,)),
            pltpu.SemaphoreType.DMA((16,)),
            pltpu.SemaphoreType.DMA((NTEN, 2)),
        ],
        compiler_params=pltpu.CompilerParams(collective_id=0, has_side_effects=True, vmem_limit_bytes=60 * 2**20),
        cost_estimate=pl.CostEstimate(flops=60_000_000_000, bytes_accessed=4_000_000, transcendentals=33_000_000),
        name="layer",
    )(qkv, gain, tokens, w_out, w_up, w_down)


def per_device(tokens, norm_gain, w_qkv, w_out, post_gain, w_up, w_down):
    base = tokens.astype(f32)
    normed = layer_norm(base, norm_gain).astype(bf16)
    qkv = lax.dot_general(w_qkv.reshape(w_qkv.shape[0], -1), normed, (((0,), (1,)), ((), ())), preferred_element_type=f32)
    scale = jnp.concatenate([jnp.full((192, 1), 1.4426950408889634 / HD**0.5, f32), jnp.ones((384, 1), f32)])
    qkv = jnp.pad((qkv * scale).astype(bf16), ((0, 0), (0, PAD - ROWS))).reshape(3, 4, HD, PAD)
    return layer(qkv, post_gain[None, :], tokens, w_out, w_up, w_down)[:ROWS]


def solution(mesh):
    placed = (P("seq", None), P(), P(None, None, "tensor"), P("tensor", None), P(), P(None, "tensor"), P("tensor", None))
    return jax.shard_map(per_device, mesh=mesh, in_specs=placed, out_specs=P("seq", None), check_vma=False)
```

```python
import functools

import jax
import jax.numpy as jnp
from jax import lax
from jax.experimental import pallas as pl
from jax.experimental.pallas import tpu as pltpu
from jax.sharding import PartitionSpec as P

HD = 48
ROWS = 720
PAD = 768
NSEQ = 16
NTEN = 8
W = 256
NC = PAD // W
f32 = jnp.float32
bf16 = jnp.bfloat16
MESH = pl.DeviceIdType.MESH

OWN, A, B, C, F, D, E, G = range(8)
DZ = (0, 0, 0, 1, 0, 1, 1, 1)
DY = (0, 3, 1, 0, 2, 3, 1, 2)
ARRIVE = {
    0: ((0, OWN, 1),), 1: ((0, A, 0), (0, B, 0), (0, C, 0)), 4: ((0, A, 1),), 5: ((0, B, 1),), 6: ((0, C, 1), (0, D, 0), (0, E, 0)),
       9: ((0, D, 1),), 10: ((0, E, 1),), 11: ((0, F, 0),), 12: ((0, G, 0),), 13: ((0, F, 1),),
    14: ((0, G, 1),), 15: ((1, OWN, 1),), 16: ((1, A, 0), (1, B, 0), (1, C, 0)), 20: ((1, A, 1),), 21: ((1, B, 1), (1, D, 0), (1, E, 0)),
    22: ((1, C, 1),), 23: ((1, D, 1),), 24: ((1, E, 1), (1, F, 0)), 25: ((1, G, 0), (1, F, 1)), 26: ((1, G, 1),),
}


def layer_norm(values, gain):
    mean = jnp.mean(values, axis=-1, keepdims=True)
    centred = values - mean
    var = jnp.mean(centred * centred, axis=-1, keepdims=True)
    return centred * lax.rsqrt(var + 1e-05) * gain


def layer_kernel(gain_in, gain, tokens, w_in, w_out, w_up, w_down, out, qt, wq, kt, vt, s0, s1, p0, p1, acc, peak, att, wf, tok, wu, wd,
                 mixed, post, term, ra, rb, ra2, rb2, sa2, sb2, rr, sr, ssem, rsem, tsend, trecv, wsend, wrecv, lsem,
                 qsend, rarecv, rbrecv, ra2recv, rb2recv, rrrecv, gsend, grecv):
    me = lax.axis_index("seq")
    ti = lax.axis_index("tensor")
    zh, yy, core = lax.div(me, 8), lax.rem(lax.div(me, 2), 4), lax.rem(me, 2)
    zl, xx = lax.div(ti, 4), lax.rem(ti, 4)

    def seq_id(off, other=0):
        return (lax.rem(zh + DZ[off], 2) * 4 + lax.rem(yy + DY[off], 4)) * 2 + lax.rem(core + other, 2)

    def ten_id(dz, dx):
        return lax.rem(zl + dz, 2) * 4 + lax.rem(xx + dx, 4)

    seq_near = [seq_id(OWN, 1), seq_id(A), seq_id(B), seq_id(C)]
    ten_near = [ten_id(0, 1), ten_id(0, 3), ten_id(1, 0), ten_id(1, 1), ten_id(1, 3)]
    ten_all = [ten_id(0, 1), ten_id(0, 3), ten_id(0, 2), ten_id(1, 0), ten_id(1, 1), ten_id(1, 3)]
    loads = [
        pltpu.make_async_copy(tokens, tok.at[0:ROWS], lsem.at[0]),
        pltpu.make_async_copy(w_in, wq, lsem.at[1]),
        pltpu.make_async_copy(w_up, wu, lsem.at[2]),
        pltpu.make_async_copy(w_down, wd, lsem.at[3]),
    ]
    loads += [
        pltpu.make_async_copy(
            w_out.at[h * HD : (h + 1) * HD], wf.at[pl.ds(pl.multiple_of(h * 384 + ti * HD, 16), HD)], lsem.at[4 + h]
        )
        for h in range(4)
    ]
    for c in loads:
        c.start()
    barrier = pltpu.get_barrier_semaphore()
    for d in seq_near:
        pl.semaphore_signal(barrier, inc=1, device_id={"seq": d}, device_id_type=MESH)
    for d in ten_all:
        pl.semaphore_signal(barrier, inc=1, device_id={"tensor": d}, device_id_type=MESH)

    lane = lax.broadcasted_iota(jnp.int32, (16, PAD), 1)
    row = lax.broadcasted_iota(jnp.int32, (16, PAD), 0)
    ones = jnp.where((row == 0) & (lane < ROWS), 1.0, 0.0).astype(bf16)

    def fill(s, _):
        for h in range(4):
            vt[s, h, HD:64, :] = ones
        return 0

    lax.fori_loop(0, NSEQ, fill, 0)
    peak[0:4] = jnp.full((4, 16, PAD), -1e30, f32)
    peak[4:6] = jnp.ones((2, 16, PAD), f32)
    acc[...] = jnp.zeros(acc.shape, f32)
    p0[ROWS:PAD, :] = jnp.zeros((PAD - ROWS, PAD), bf16)
    p1[...] = jnp.zeros((PAD, PAD), bf16)
    tok[ROWS:PAD, :] = jnp.zeros((PAD - ROWS, 1536), bf16)
    loads[0].wait()

    def norm(c, _):
        rows = pl.ds(pl.multiple_of(c * W, W), W)
        post[rows, :] = layer_norm(tok[rows, :].astype(f32), gain_in[...]).astype(bf16)
        return 0

    lax.fori_loop(0, NC, norm, 0)
    loads[1].wait()

    def heads_of(part):
        return lax.dot_general(wq[part], post[...], (((1,), (1,)), ((), ())), preferred_element_type=f32)

    keys = heads_of(1).astype(bf16)
    values = heads_of(2).astype(bf16)
    for h in range(4):
        kt[me, h] = keys[h * HD : (h + 1) * HD]
        vt[me, h, 0:HD, :] = values[h * HD : (h + 1) * HD]
    pl.semaphore_wait(barrier, len(seq_near) + len(ten_all))

    sent = [[], []]

    def block_ref(piece, slot, hp):
        ref = kt if piece == 0 else vt
        return ref.at[slot, 2 * hp : 2 * hp + 2, 0:HD]

    def seq_copy(piece, slot, hp, dest, index):
        return pltpu.make_async_remote_copy(
            src_ref=block_ref(piece, slot, hp), dst_ref=block_ref(piece, slot, hp), send_sem=ssem.at[hp, index],
            recv_sem=rsem.at[slot, hp, piece], device_id={"seq": dest}, device_id_type=MESH,
        )

    def send(piece, slot, hp, dest):
        c = seq_copy(piece, slot, hp, dest, len(sent[hp]))
        c.start()
        sent[hp].append(piece)

    def send_own(hp):
        for piece in (0, 1):
            for d in (seq_id(B), seq_id(A), seq_id(C), seq_id(OWN, 1)):
                send(piece, me, hp, d)

    def arrive(hp, off, other):
        slot = seq_id(off, other)
        for piece in (0, 1):
            seq_copy(piece, slot, hp, me, 0).wait_recv()
        if other:
            return
        if off in (D, E):
            onward(hp, off)
        for piece in (0, 1):
            send(piece, slot, hp, seq_id(OWN, 1))

    def onward(hp, off):
        if off in (A, D):
            send(0, seq_id(off), hp, seq_id(B))
        else:
            send(1, seq_id(off), hp, seq_id(A))

    def spread(hp):
        slot = seq_id(C)
        for piece in (0, 1):
            for d in (seq_id(B), seq_id(A)):
                send(piece, slot, hp, d)
        onward(hp, A)
        onward(hp, B)

    tsent = []

    def head_ref(src, head):
        return att.at[pl.ds(pl.multiple_of(head * 384 + src * HD, 16), HD)]

    def ten_copy(src, head, dest, index):
        return pltpu.make_async_remote_copy(
            src_ref=head_ref(src, head), dst_ref=head_ref(src, head), send_sem=tsend.at[index],
            recv_sem=trecv.at[src, head], device_id={"tensor": dest}, device_id_type=MESH,
        )

    def ten_start(src, head, dest):
        c = ten_copy(src, head, dest, len(tsent))
        c.start()
        tsent.append(0)

    def finish(heads):
        for h in heads:
            att[pl.ds(pl.multiple_of(h * 384 + ti * HD, 16), HD), :] = (acc[h, 0:HD, :] / acc[h, HD : HD + 1, :]).astype(bf16)
        for h in heads:
            for d in ten_near:
                ten_start(ti, h, d)

    def ten_wait(src, head):
        ten_copy(src, head, ti, 0).wait_recv()

    def relay(head):
        for src, dest in ((ten_id(0, 3), ten_id(0, 1)), (ten_id(1, 1), ten_id(0, 3))):
            ten_wait(src, head)
            ten_start(src, head, dest)

    def collect(head):
        for src in (ten_id(0, 1), ten_id(1, 3), ten_id(1, 0), ten_id(0, 2), ten_id(1, 2)):
            ten_wait(src, head)

    wsent = []

    def w_copy(src, half, other, dest, index):
        at = lax.rem(core + other, 2)
        ref = wf.at[pl.ds(pl.multiple_of((at * 2 + half) * 384 + src * HD, 16), HD)]
        return pltpu.make_async_remote_copy(
            src_ref=ref, dst_ref=ref, send_sem=wsend.at[index], recv_sem=wrecv.at[src, other, half],
            device_id=dest, device_id_type=MESH,
        )

    def w_start(src, half, dest, index_other=0):
        at = core
        ref = wf.at[pl.ds(pl.multiple_of((at * 2 + half) * 384 + src * HD, 16), HD)]
        pltpu.make_async_remote_copy(
            src_ref=ref, dst_ref=ref, send_sem=wsend.at[len(wsent)], recv_sem=wrecv.at[src, index_other, half],
            device_id=dest, device_id_type=MESH,
        ).start()
        wsent.append(0)

    def w_wait(src, half, other):
        w_copy(src, half, other, {"tensor": ti}, 0).wait_recv()

    def w_share(src):
        for half in (0, 1):
            w_start(src, half, {"seq": seq_id(OWN, 1)}, 1)

    def w_own():
        for c in loads[4:]:
            c.wait()
        for half in (0, 1):
            for d in (ten_id(0, 1), ten_id(0, 3), ten_id(1, 0)):
                w_start(ti, half, {"tensor": d})

    def w_relay(dz):
        left, right = ten_id(dz, 3), ten_id(dz, 1)
        for src in (left, right):
            for half in (0, 1):
                w_wait(src, half, 0)
        w_start(left, 0, {"tensor": ten_id(0, 1)})
        w_start(right, 1, {"tensor": ten_id(0, 3)})
        w_share(left)
        w_share(right)

    def w_cross():
        src = ten_id(1, 0)
        for half in (0, 1):
            w_wait(src, half, 0)
            for d in (ten_id(0, 1), ten_id(0, 3)):
                w_start(src, half, {"tensor": d})
        w_share(src)

    def w_far(dz):
        src = ten_id(dz, 2)
        for half in (0, 1):
            w_wait(src, half, 0)
        w_share(src)

    def w_collect():
        for dz in (0, 1):
            for dx in range(4):
                if (dz, dx) != (0, 0):
                    for half in (0, 1):
                        w_wait(ten_id(dz, dx), half, 1)

    S, Pw = (s0, s1), (p0, p1)

    def slot_at(pos):
        mid, late = (pos >= 2).astype(jnp.int32), (pos >= 8).astype(jnp.int32)
        q, r = lax.rem(pos + 4, 6), lax.rem(pos, 4)
        chip = mid * (1 - late) * (1 + lax.rem(q, 3)) + late * (2 * lax.div(pos, 4) + lax.rem(r, 2))
        other = (1 - mid) * pos + mid * (1 - late) * lax.div(q, 3) + late * lax.div(r, 2)
        far = (chip >= 6).astype(jnp.int32)
        dy = (1 - far) * lax.rem(3 * lax.rem(chip, 3), 5) + 2 * far
        dz = (1 - far) * lax.div(chip, 3) + far * (chip - 6)
        return (lax.rem(zh + dz, 2) * 4 + lax.rem(yy + dy, 4)) * 2 + lax.rem(core + other, 2)

    def score_pieces(slot, head, par, top):
        def mk(c, half):
            cs = slice(c * W, (c + 1) * W)

            def go():
                lo = half * 384
                n = 384 if half == 0 else ROWS - 384
                s = lax.dot_general(
                    kt[slot, head, :, lo : lo + 384], qt[head, :, cs], (((0,), (0,)), ((), ())), preferred_element_type=f32
                )[0:n]
                S[par][lo : lo + n, cs] = s
                b = jnp.max(s.reshape(-1, 8, W), axis=0)
                top[c] = b if c not in top else jnp.maximum(top[c], b)

            return go

        return [mk(c, half) for c in range(NC) for half in (0, 1)]

    def weight_pieces(par, now):
        def mk(c, r):
            cs = slice(c * W, (c + 1) * W)

            def go():
                Pw[par][r : r + 240, cs] = jnp.exp2(S[par][r : r + 240, cs] - now[c]).astype(bf16)

            return go

        return [mk(c, r) for c in range(NC) for r in (0, 240, 480)]

    def value_pieces(slot, head, par, factor):
        def mk(c):
            cs = slice(c * W, (c + 1) * W)

            def go():
                acc[head, :, cs] = acc[head, :, cs] * factor[c] + jnp.dot(
                    vt[slot, head], Pw[par][:, cs], preferred_element_type=f32
                )

            return go

        return [mk(c) for c in range(NC)]

    def interleave(*lists):
        events = []
        for k, items in enumerate(lists):
            for j, x in enumerate(items):
                events.append(((j + 0.5) / len(items), k, x))
        events.sort(key=lambda e: (e[0], e[1]))
        for _, _, x in events:
            x()

    def keep_top(head, top):
        for c in range(NC):
            peak[head, 8:16, c * W : (c + 1) * W] = top[c]

    def item(n):
        n = lax.rem(n, 64)
        late = (n >= 44).astype(jnp.int32)
        last = (n >= 54).astype(jnp.int32)
        pos = (1 - late) * lax.div(lax.rem(n, 32), 2) + late * (n - 38 - 10 * last)
        head = (1 - late) * (2 * lax.div(n, 32) + lax.rem(n, 2)) + late * (2 + last)
        return slot_at(pos), head

    def step(t, held):
        def events(at):
            for hp, off, other in ARRIVE.get(at, ()):
                arrive(hp, off, other)
            if at == 1:
                spread(0)
            if at == 5:
                w_cross()
                w_relay(0)
            if at == 7:
                send_own(1)
            if at == 12:
                w_relay(1)
                w_far(0)
            if at == 15:
                w_far(1)
            if at == 16:
                spread(1)
            if at == 17:
                finish((0, 1))
            if at == 24:
                relay(0)
                relay(1)
            if at == 30:
                collect(0)
                collect(1)
                w_collect()
            if at == 28:
                finish((2,))

        at_all = sorted(set(ARRIVE) | {1, 5, 7, 12, 15, 16, 17, 24, 28, 30})

        def search(lo, hi):
            inside = [at for at in at_all if lo <= at < hi]
            if not inside:
                return
            if hi - lo == 1:
                events(lo)
                return
            mid = (lo + hi) // 2
            for a, b in ((lo, mid), (mid, hi)):
                if any(a <= at < b for at in inside):
                    test = t < mid if a == lo else t >= mid
                    pl.when(test)(functools.partial(search, a, b))

        search(0, 32)
        slots = {q: item(2 * t + q) for q in (1, 2)}
        slots[-1], slots[0] = (held[0], held[1]), (held[2], held[3])
        for k in (0, 1):
            (slot_p, head_p), (slot, head), (slot_n, head_n) = slots[k - 1], slots[k], slots[k + 1]
            now, factor_p = {}, {}
            for c in range(NC):
                cs = slice(c * W, (c + 1) * W)
                factor_p[c] = peak[5 - k, 0:1, cs]
                old = peak[head, 0:1, cs]
                now[c] = jnp.maximum(old, jnp.max(peak[head, 8:16, cs], axis=0, keepdims=True))
                peak[4 + k, 0:1, cs] = jnp.exp2(old - now[c])
                peak[head, 0:1, cs] = now[c]
            top = {}
            interleave(
                score_pieces(slot_n, head_n, 1 - k, top),
                weight_pieces(k, now),
                value_pieces(slot_p, head_p, 1 - k, factor_p),
            )
            keep_top(head_n, top)
        return (*slots[1], *slots[2])

    send_own(0)
    queries = (heads_of(0) * (1.4426950408889634 / HD**0.5)).astype(bf16)
    for h in range(4):
        qt[h] = queries[h * HD : (h + 1) * HD]
    w_own()
    top = {}
    for x in score_pieces(me, 0, 0, top):
        x()
    keep_top(0, top)
    lax.fori_loop(0, 32, step, (me, me * 0, me, me * 0))
    for x in value_pieces(slot_at(me * 0 + 15), 3, 1, {c: peak[5, 0:1, c * W : (c + 1) * W] for c in range(NC)}):
        x()
    finish((3,))
    relay(2)
    for c in loads[2:4]:
        c.wait()

    def project(c, _):
        cols = pl.ds(pl.multiple_of(c * W, W), W)
        mixed[cols, :] = tok[cols, :].astype(f32) + lax.dot_general(
            att[0:768, cols], wf[0:768, :], (((0,), (0,)), ((), ())), preferred_element_type=f32
        )
        return 0

    lax.fori_loop(0, NC, project, 0)
    relay(3)
    collect(2)
    collect(3)

    def complete(c, _):
        cols = pl.ds(pl.multiple_of(c * W, W), W)
        m = mixed[cols, :] + lax.dot_general(
            att[768:1536, cols], wf[768:1536, :], (((0,), (0,)), ((), ())), preferred_element_type=f32
        )
        mixed[cols, :] = m
        post[cols, :] = layer_norm(m, gain[...]).astype(bf16)
        return 0

    lax.fori_loop(0, NC, complete, 0)

    def rows_of(t, half=0, n=48):
        return pl.ds(pl.multiple_of(t * 96 + half * 48, 16), n)

    qsent = []

    def q_copy(src_ref, dst_ref, recv, dest, index):
        return pltpu.make_async_remote_copy(
            src_ref=src_ref, dst_ref=dst_ref, send_sem=qsend.at[index], recv_sem=recv,
            device_id={"tensor": dest}, device_id_type=MESH,
        )

    def q_start(src_ref, dst_ref, recv, dest):
        q_copy(src_ref, dst_ref, recv, dest, len(qsent)).start()
        qsent.append(0)

    def q_wait(ref, recv):
        q_copy(ref, ref, recv, ti, 0).wait_recv()

    def part(t, half):
        return term[rows_of(t, half), :].astype(f32)

    for dx in (2, 3, 1, 0):
        t0, t1 = ten_id(0, dx), ten_id(1, dx)
        both = jnp.concatenate([post[rows_of(t0, 0, 96), :], post[rows_of(t1, 0, 96), :]], axis=0)
        u = jnp.dot(both, wu[...], preferred_element_type=f32)
        h = jax.nn.gelu(u, approximate=True).astype(bf16)
        y = jnp.dot(h, wd[...], preferred_element_type=f32).astype(bf16)
        term[rows_of(t0, 0, 96), :] = y[0:96]
        term[rows_of(t1, 0, 96), :] = y[96:192]
        q_start(term.at[rows_of(t1, 1)], rb.at[dx], rbrecv.at[dx], ten_id(1, 0))
        if dx == 2:
            q_start(term.at[rows_of(t0)], rr.at[0], rrrecv.at[0], ten_id(0, 1))
            q_start(term.at[rows_of(t1)], rr.at[1], rrrecv.at[1], ten_id(0, 3))
        if dx == 1:
            q_start(term.at[rows_of(t1)], ra.at[1, 0], rarecv.at[1, 0], t0)
        if dx == 3:
            q_start(term.at[rows_of(t0)], ra.at[0, 1], rarecv.at[0, 1], t0)
    for k, dx in ((0, 1), (1, 3)):
        q_wait(rr.at[k], rrrecv.at[k])
        sr[k] = (part(ten_id(k, dx), 0) + rr[k].astype(f32)).astype(bf16)
        q_start(sr.at[k], ra.at[k, k], rarecv.at[k, k], ten_id(0, dx))
    for dx in (2, 1, 3):
        q_wait(rb.at[dx], rbrecv.at[dx])
        sb2[dx - 1] = (part(ten_id(0, dx), 1) + rb[dx].astype(f32)).astype(bf16)
        q_start(sb2.at[dx - 1], rb2.at[3 - dx], rb2recv.at[3 - dx], ten_id(0, dx))
    total = part(ten_id(1, 0), 0)
    for k in range(2):
        q_wait(ra.at[1, k], rarecv.at[1, k])
        total = total + ra[1, k].astype(f32)
    sa2[...] = total.astype(bf16)
    q_start(sa2, ra2, ra2recv.at[0], ten_id(1, 0))

    gsent = []

    def g_copy(t, half, dest, index):
        ref = out.at[rows_of(t, half)]
        return pltpu.make_async_remote_copy(
            src_ref=ref, dst_ref=ref, send_sem=gsend.at[index], recv_sem=grecv.at[t, half],
            device_id={"tensor": dest}, device_id_type=MESH,
        )

    def g_start(t, half, dest):
        g_copy(t, half, dest, len(gsent)).start()
        gsent.append(0)

    def g_wait(t, half):
        g_copy(t, half, ti, 0).wait_recv()

    q_wait(rb.at[0], rbrecv.at[0])
    total = mixed[rows_of(ti, 1), :] + part(ti, 1) + rb[0].astype(f32)
    for k in range(3):
        q_wait(rb2.at[k], rb2recv.at[k])
        total = total + rb2[k].astype(f32)
    out[rows_of(ti, 1), :] = total.astype(bf16)
    g_start(ti, 1, ten_id(1, 0))
    total = mixed[rows_of(ti, 0), :] + part(ti, 0)
    for k in range(2):
        q_wait(ra.at[0, k], rarecv.at[0, k])
        total = total + ra[0, k].astype(f32)
    q_wait(ra2, ra2recv.at[0])
    total = total + ra2[...].astype(f32)
    out[rows_of(ti, 0), :] = total.astype(bf16)
    for dx in (1, 3, 2):
        g_start(ti, 0, ten_id(0, dx))
    g_start(ti, 0, ten_id(1, 0))
    for dx in (1, 3):
        g_start(ti, 1, ten_id(0, dx))
    g_wait(ten_id(1, 0), 1)
    for dx in (1, 3):
        g_start(ten_id(1, 0), 1, ten_id(0, dx))
    for dx in (1, 3):
        g_wait(ten_id(0, dx), 0)
        g_start(ten_id(0, dx), 0, ten_id(1, 0))
    g_wait(ten_id(0, 3), 1)
    g_start(ten_id(0, 3), 1, ten_id(0, 1))
    g_wait(ten_id(0, 2), 0)
    g_start(ten_id(0, 2), 0, ten_id(1, 0))
    g_wait(ten_id(1, 1), 1)
    g_start(ten_id(1, 1), 1, ten_id(0, 3))
    g_wait(ten_id(1, 0), 0)
    for t, half in (((0, 1), 1), ((0, 2), 1), ((1, 3), 1), ((1, 2), 1), ((1, 1), 0), ((1, 3), 0), ((1, 2), 0)):
        g_wait(ten_id(*t), half)

    for hp in (0, 1):
        for index, piece in enumerate(sent[hp]):
            seq_copy(piece, me, hp, me, index).wait_send()
    for index in range(len(tsent)):
        ten_copy(ti, 0, ti, index).wait_send()
    for index in range(len(wsent)):
        w_copy(ti, 0, 0, {"tensor": ti}, index).wait_send()
    for index in range(len(qsent)):
        q_copy(sa2, ra2, ra2recv.at[0], ti, index).wait_send()
    for index in range(len(gsent)):
        g_copy(ti, 0, ti, index).wait_send()


def layer(gain_in, gain, tokens, w_in, w_out, w_up, w_down):
    vmem = pl.BlockSpec(memory_space=pltpu.VMEM)
    hbm = pl.BlockSpec(memory_space=pl.ANY)
    D = tokens.shape[1]
    return pl.pallas_call(
        layer_kernel,
        out_shape=jax.ShapeDtypeStruct((PAD, D), bf16),
        in_specs=[vmem, vmem, hbm, hbm, hbm, hbm, hbm],
        out_specs=vmem,
        scratch_shapes=[
            pltpu.VMEM((4, HD, PAD), bf16),
            pltpu.VMEM((3, 192, D), bf16),
            pltpu.VMEM((NSEQ, 4, HD, PAD), bf16),
            pltpu.VMEM((NSEQ, 4, 64, PAD), bf16),
            pltpu.VMEM((ROWS, PAD), f32),
            pltpu.VMEM((ROWS, PAD), f32),
            pltpu.VMEM((PAD, PAD), bf16),
            pltpu.VMEM((PAD, PAD), bf16),
            pltpu.VMEM((4, 64, PAD), f32),
            pltpu.VMEM((6, 16, PAD), f32),
            pltpu.VMEM((D, PAD), bf16),
            pltpu.VMEM((D, D), bf16),
            pltpu.VMEM((PAD, D), bf16),
            pltpu.VMEM((D, 768), bf16),
            pltpu.VMEM((768, D), bf16),
            pltpu.VMEM((PAD, D), f32),
            pltpu.VMEM((PAD, D), bf16),
            pltpu.VMEM((PAD, D), bf16),
            pltpu.VMEM((2, 2, 48, D), bf16),
            pltpu.VMEM((4, 48, D), bf16),
            pltpu.VMEM((48, D), bf16),
            pltpu.VMEM((3, 48, D), bf16),
            pltpu.VMEM((48, D), bf16),
            pltpu.VMEM((3, 48, D), bf16),
            pltpu.VMEM((2, 48, D), bf16),
            pltpu.VMEM((2, 48, D), bf16),
            pltpu.SemaphoreType.DMA((2, 32)),
            pltpu.SemaphoreType.DMA((NSEQ, 2, 2)),
            pltpu.SemaphoreType.DMA((32,)),
            pltpu.SemaphoreType.DMA((NTEN, 4)),
            pltpu.SemaphoreType.DMA((32,)),
            pltpu.SemaphoreType.DMA((NTEN, 2, 2)),
            pltpu.SemaphoreType.DMA((8,)),
            pltpu.SemaphoreType.DMA((16,)),
            pltpu.SemaphoreType.DMA((2, 2)),
            pltpu.SemaphoreType.DMA((4,)),
            pltpu.SemaphoreType.DMA((1,)),
            pltpu.SemaphoreType.DMA((3,)),
            pltpu.SemaphoreType.DMA((2,)),
            pltpu.SemaphoreType.DMA((16,)),
            pltpu.SemaphoreType.DMA((NTEN, 2)),
        ],
        compiler_params=pltpu.CompilerParams(
            collective_id=0, has_side_effects=True, vmem_limit_bytes=60 * 2**20,
        ),
        cost_estimate=pl.CostEstimate(flops=60_000_000_000, bytes_accessed=4_000_000, transcendentals=33_000_000),
        name="layer",
    )(gain_in, gain, tokens, w_in, w_out, w_up, w_down)


def per_device(tokens, norm_gain, w_qkv, w_out, post_gain, w_up, w_down):
    w_in = jnp.transpose(w_qkv, (1, 2, 0))
    return layer(norm_gain[None, :], post_gain[None, :], tokens, w_in, w_out, w_up, w_down)[:ROWS]


def solution(mesh):
    placed = (P("seq", None), P(), P(None, None, "tensor"), P("tensor", None), P(), P(None, "tensor"), P("tensor", None))
    return jax.shard_map(per_device, mesh=mesh, in_specs=placed, out_specs=P("seq", None), check_vma=False)
```

```python
import functools

import jax
import jax.numpy as jnp
from jax import lax
from jax.experimental import pallas as pl
from jax.experimental.pallas import tpu as pltpu
from jax.sharding import PartitionSpec as P

HD = 48
ROWS = 720
PAD = 768
NSEQ = 16
NTEN = 8
W = 256
NC = PAD // W
f32 = jnp.float32
bf16 = jnp.bfloat16
MESH = pl.DeviceIdType.MESH

OWN, A, B, C, F, D, E, G = range(8)
DZ = (0, 0, 0, 1, 0, 1, 1, 1)
DY = (0, 3, 1, 0, 2, 3, 1, 2)
ARRIVE = {
    0: ((0, OWN, 1),), 4: ((0, A, 1),), 5: ((0, B, 1),), 6: ((0, C, 1), (0, D, 0), (0, E, 0)),
    9: ((0, D, 1), (0, F, 0)), 10: ((0, E, 1),), 12: ((0, G, 0),), 13: ((0, F, 1),), 14: ((0, G, 1),),
    15: ((1, OWN, 1),), 16: ((1, A, 0), (1, B, 0), (1, C, 0)), 20: ((1, A, 1),), 21: ((1, B, 1), (1, D, 0), (1, E, 0)),
    22: ((1, C, 1),), 23: ((1, D, 1),), 24: ((1, E, 1), (1, F, 0)), 25: ((1, G, 0), (1, F, 1)), 26: ((1, G, 1),),
}


def layer_norm(values, gain):
    mean = jnp.mean(values, axis=-1, keepdims=True)
    centred = values - mean
    var = jnp.mean(centred * centred, axis=-1, keepdims=True)
    return centred * lax.rsqrt(var + 1e-05) * gain


def layer_kernel(gain_in, gain, tokens, w_in, w_out, w_up, w_down, out, qt, wq, kt, vt, s0, s1, p0, p1, acc, peak, att, wf, tok, wu, wd,
                 mixed, post, term, ra, rb, ra2, rb2, sa2, sb2, rr, sr, ssem, rsem, tsend, trecv, wsend, wrecv, lsem,
                 qsend, rarecv, rbrecv, ra2recv, rb2recv, rrrecv, gsend, grecv):
    me = lax.axis_index("seq")
    ti = lax.axis_index("tensor")
    zh, yy, core = lax.div(me, 8), lax.rem(lax.div(me, 2), 4), lax.rem(me, 2)
    zl, xx = lax.div(ti, 4), lax.rem(ti, 4)

    def seq_id(off, other=0):
        return (lax.rem(zh + DZ[off], 2) * 4 + lax.rem(yy + DY[off], 4)) * 2 + lax.rem(core + other, 2)

    def ten_id(dz, dx):
        return lax.rem(zl + dz, 2) * 4 + lax.rem(xx + dx, 4)

    seq_near = [seq_id(OWN, 1), seq_id(A), seq_id(B), seq_id(C)]
    ten_near = [ten_id(0, 1), ten_id(0, 3), ten_id(1, 0), ten_id(1, 1), ten_id(1, 3)]
    ten_all = [ten_id(0, 1), ten_id(0, 3), ten_id(0, 2), ten_id(1, 0), ten_id(1, 1), ten_id(1, 3)]
    loads = [
        pltpu.make_async_copy(tokens, tok.at[0:ROWS], lsem.at[0]),
        pltpu.make_async_copy(w_in, wq, lsem.at[1]),
        pltpu.make_async_copy(w_up, wu, lsem.at[2]),
        pltpu.make_async_copy(w_down, wd, lsem.at[3]),
    ]
    loads += [
        pltpu.make_async_copy(
            w_out.at[h * HD : (h + 1) * HD], wf.at[pl.ds(pl.multiple_of(h * 384 + ti * HD, 16), HD)], lsem.at[4 + h]
        )
        for h in range(4)
    ]
    for c in loads:
        c.start()
    barrier = pltpu.get_barrier_semaphore()
    for d in seq_near:
        pl.semaphore_signal(barrier, inc=1, device_id={"seq": d}, device_id_type=MESH)
    for d in ten_all:
        pl.semaphore_signal(barrier, inc=1, device_id={"tensor": d}, device_id_type=MESH)

    lane = lax.broadcasted_iota(jnp.int32, (16, PAD), 1)
    row = lax.broadcasted_iota(jnp.int32, (16, PAD), 0)
    ones = jnp.where((row == 0) & (lane < ROWS), 1.0, 0.0).astype(bf16)

    def fill(s, _):
        for h in range(4):
            vt[s, h, HD:64, :] = ones
        return 0

    lax.fori_loop(0, NSEQ, fill, 0)
    peak[0:4] = jnp.full((4, 16, PAD), -1e30, f32)
    peak[4:6] = jnp.ones((2, 16, PAD), f32)
    acc[...] = jnp.zeros(acc.shape, f32)
    p0[ROWS:PAD, :] = jnp.zeros((PAD - ROWS, PAD), bf16)
    p1[...] = jnp.zeros((PAD, PAD), bf16)
    tok[ROWS:PAD, :] = jnp.zeros((PAD - ROWS, 1536), bf16)
    loads[0].wait()

    def norm(c, _):
        rows = pl.ds(pl.multiple_of(c * W, W), W)
        post[rows, :] = layer_norm(tok[rows, :].astype(f32), gain_in[...]).astype(bf16)
        return 0

    lax.fori_loop(0, NC, norm, 0)
    loads[1].wait()

    def heads_of(part):
        return lax.dot_general(wq[part], post[...], (((1,), (1,)), ((), ())), preferred_element_type=f32)

    keys = heads_of(1).astype(bf16)
    values = heads_of(2).astype(bf16)
    for h in range(4):
        kt[me, h] = keys[h * HD : (h + 1) * HD]
        vt[me, h, 0:HD, :] = values[h * HD : (h + 1) * HD]
    pl.semaphore_wait(barrier, len(seq_near) + len(ten_all))

    sent = [[], []]

    def block_ref(piece, slot, hp):
        ref = kt if piece == 0 else vt
        return ref.at[slot, 2 * hp : 2 * hp + 2, 0:HD]

    def seq_copy(piece, slot, hp, dest, index):
        return pltpu.make_async_remote_copy(
            src_ref=block_ref(piece, slot, hp), dst_ref=block_ref(piece, slot, hp), send_sem=ssem.at[hp, index],
            recv_sem=rsem.at[slot, hp, piece], device_id={"seq": dest}, device_id_type=MESH,
        )

    def send(piece, slot, hp, dest):
        c = seq_copy(piece, slot, hp, dest, len(sent[hp]))
        c.start()
        sent[hp].append(piece)

    def send_own(hp):
        for piece in (0, 1):
            for d in (seq_id(B), seq_id(A), seq_id(C), seq_id(OWN, 1)):
                send(piece, me, hp, d)

    def arrive(hp, off, other, pieces=(0, 1)):
        slot = seq_id(off, other)
        for piece in pieces:
            seq_copy(piece, slot, hp, me, 0).wait_recv()
        if other:
            return
        if off in (D, E):
            onward(hp, off)
        for piece in pieces:
            send(piece, slot, hp, seq_id(OWN, 1))

    def onward(hp, off):
        if off in (A, D):
            send(0, seq_id(off), hp, seq_id(B))
        else:
            send(1, seq_id(off), hp, seq_id(A))

    def spread(hp, pieces=(0, 1)):
        slot = seq_id(C)
        for piece in pieces:
            for d in (seq_id(B), seq_id(A)):
                send(piece, slot, hp, d)
        for piece in pieces:
            onward(hp, (A, B)[piece])

    tsent = []

    def head_ref(src, head):
        return att.at[pl.ds(pl.multiple_of(head * 384 + src * HD, 16), HD)]

    def ten_copy(src, head, dest, index):
        return pltpu.make_async_remote_copy(
            src_ref=head_ref(src, head), dst_ref=head_ref(src, head), send_sem=tsend.at[index],
            recv_sem=trecv.at[src, head], device_id={"tensor": dest}, device_id_type=MESH,
        )

    def ten_start(src, head, dest):
        c = ten_copy(src, head, dest, len(tsent))
        c.start()
        tsent.append(0)

    def finish(heads):
        for h in heads:
            att[pl.ds(pl.multiple_of(h * 384 + ti * HD, 16), HD), :] = (acc[h, 0:HD, :] / acc[h, HD : HD + 1, :]).astype(bf16)
        for h in heads:
            for d in ten_near:
                ten_start(ti, h, d)

    def ten_wait(src, head):
        ten_copy(src, head, ti, 0).wait_recv()

    def relay(head):
        for src, dest in ((ten_id(0, 3), ten_id(0, 1)), (ten_id(1, 1), ten_id(0, 3))):
            ten_wait(src, head)
            ten_start(src, head, dest)

    def collect(head):
        for src in (ten_id(0, 1), ten_id(1, 3), ten_id(1, 0), ten_id(0, 2), ten_id(1, 2)):
            ten_wait(src, head)

    wsent = []

    def w_copy(src, half, other, dest, index):
        at = lax.rem(core + other, 2)
        ref = wf.at[pl.ds(pl.multiple_of((at * 2 + half) * 384 + src * HD, 16), HD)]
        return pltpu.make_async_remote_copy(
            src_ref=ref, dst_ref=ref, send_sem=wsend.at[index], recv_sem=wrecv.at[src, other, half],
            device_id=dest, device_id_type=MESH,
        )

    def w_start(src, half, dest, index_other=0):
        at = core
        ref = wf.at[pl.ds(pl.multiple_of((at * 2 + half) * 384 + src * HD, 16), HD)]
        pltpu.make_async_remote_copy(
            src_ref=ref, dst_ref=ref, send_sem=wsend.at[len(wsent)], recv_sem=wrecv.at[src, index_other, half],
            device_id=dest, device_id_type=MESH,
        ).start()
        wsent.append(0)

    def w_wait(src, half, other):
        w_copy(src, half, other, {"tensor": ti}, 0).wait_recv()

    def w_share(src):
        for half in (0, 1):
            w_start(src, half, {"seq": seq_id(OWN, 1)}, 1)

    def w_own():
        for c in loads[4:]:
            c.wait()
        for half in (0, 1):
            for d in (ten_id(0, 1), ten_id(0, 3), ten_id(1, 0)):
                w_start(ti, half, {"tensor": d})

    def w_relay(dz):
        left, right = ten_id(dz, 3), ten_id(dz, 1)
        for src in (left, right):
            for half in (0, 1):
                w_wait(src, half, 0)
        w_start(left, 0, {"tensor": ten_id(0, 1)})
        w_start(right, 1, {"tensor": ten_id(0, 3)})
        w_share(left)
        w_share(right)

    def w_cross():
        src = ten_id(1, 0)
        for half in (0, 1):
            w_wait(src, half, 0)
            for d in (ten_id(0, 1), ten_id(0, 3)):
                w_start(src, half, {"tensor": d})
        w_share(src)

    def w_far(dz):
        src = ten_id(dz, 2)
        for half in (0, 1):
            w_wait(src, half, 0)
        w_share(src)

    def w_collect():
        for dz in (0, 1):
            for dx in range(4):
                if (dz, dx) != (0, 0):
                    for half in (0, 1):
                        w_wait(ten_id(dz, dx), half, 1)

    S, Pw = (s0, s1), (p0, p1)

    def slot_at(pos):
        mid, late = (pos >= 2).astype(jnp.int32), (pos >= 8).astype(jnp.int32)
        q, r = lax.rem(pos + 4, 6), lax.rem(pos, 4)
        chip = mid * (1 - late) * (1 + lax.rem(q, 3)) + late * (2 * lax.div(pos, 4) + lax.rem(r, 2))
        other = (1 - mid) * pos + mid * (1 - late) * lax.div(q, 3) + late * lax.div(r, 2)
        far = (chip >= 6).astype(jnp.int32)
        dy = (1 - far) * lax.rem(3 * lax.rem(chip, 3), 5) + 2 * far
        dz = (1 - far) * lax.div(chip, 3) + far * (chip - 6)
        return (lax.rem(zh + dz, 2) * 4 + lax.rem(yy + dy, 4)) * 2 + lax.rem(core + other, 2)

    def score_pieces(slot, head, par, top):
        def mk(c, half):
            cs = slice(c * W, (c + 1) * W)

            def go():
                lo = half * 384
                n = 384 if half == 0 else ROWS - 384
                s = lax.dot_general(
                    kt[slot, head, :, lo : lo + 384], qt[head, :, cs], (((0,), (0,)), ((), ())), preferred_element_type=f32
                )[0:n]
                S[par][lo : lo + n, cs] = s
                b = jnp.max(s.reshape(-1, 8, W), axis=0)
                top[c] = b if c not in top else jnp.maximum(top[c], b)

            return go

        return [mk(c, half) for c in range(NC) for half in (0, 1)]

    def weight_pieces(par, now):
        def mk(c, r):
            cs = slice(c * W, (c + 1) * W)

            def go():
                Pw[par][r : r + 240, cs] = jnp.exp2(S[par][r : r + 240, cs] - now[c]).astype(bf16)

            return go

        return [mk(c, r) for c in range(NC) for r in (0, 240, 480)]

    def value_pieces(slot, head, par, factor):
        def mk(c):
            cs = slice(c * W, (c + 1) * W)

            def go():
                acc[head, :, cs] = acc[head, :, cs] * factor[c] + jnp.dot(
                    vt[slot, head], Pw[par][:, cs], preferred_element_type=f32
                )

            return go

        return [mk(c) for c in range(NC)]

    def interleave(*lists):
        events = []
        for k, items in enumerate(lists):
            for j, x in enumerate(items):
                events.append(((j + 0.5) / len(items), k, x))
        events.sort(key=lambda e: (e[0], e[1]))
        for _, _, x in events:
            x()

    def keep_top(head, top):
        for c in range(NC):
            peak[head, 8:16, c * W : (c + 1) * W] = top[c]

    def item(n):
        n = lax.rem(n, 64)
        late = (n >= 44).astype(jnp.int32)
        last = (n >= 54).astype(jnp.int32)
        pos = (1 - late) * lax.div(lax.rem(n, 32), 2) + late * (n - 38 - 10 * last)
        head = (1 - late) * (2 * lax.div(n, 32) + lax.rem(n, 2)) + late * (2 + last)
        return slot_at(pos), head

    def step(t, held):
        def events(at):
            for hp, off, other in ARRIVE.get(at, ()):
                arrive(hp, off, other)
            if at in (1, 2):
                for off in (A, B, C):
                    arrive(0, off, 0, (at - 1,))
                spread(0, (at - 1,))
            if at == 5:
                w_cross()
                w_relay(0)
            if at == 7:
                send_own(1)
            if at == 12:
                w_relay(1)
                w_far(0)
            if at == 15:
                w_far(1)
            if at == 16:
                spread(1)
            if at == 17:
                finish((0, 1))
            if at == 24:
                relay(0)
                relay(1)
            if at == 30:
                collect(0)
                collect(1)
                w_collect()
            if at == 28:
                finish((2,))

        at_all = sorted(set(ARRIVE) | {1, 2, 5, 7, 12, 15, 16, 17, 24, 28, 30})

        def search(lo, hi):
            inside = [at for at in at_all if lo <= at < hi]
            if not inside:
                return
            if hi - lo == 1:
                events(lo)
                return
            mid = (lo + hi) // 2
            for a, b in ((lo, mid), (mid, hi)):
                if any(a <= at < b for at in inside):
                    test = t < mid if a == lo else t >= mid
                    pl.when(test)(functools.partial(search, a, b))

        search(0, 32)
        slots = {q: item(2 * t + q) for q in (1, 2)}
        slots[-1], slots[0] = (held[0], held[1]), (held[2], held[3])
        for k in (0, 1):
            (slot_p, head_p), (slot, head), (slot_n, head_n) = slots[k - 1], slots[k], slots[k + 1]
            now, factor_p = {}, {}
            for c in range(NC):
                cs = slice(c * W, (c + 1) * W)
                factor_p[c] = peak[5 - k, 0:1, cs]
                old = peak[head, 0:1, cs]
                now[c] = jnp.maximum(old, jnp.max(peak[head, 8:16, cs], axis=0, keepdims=True))
                peak[4 + k, 0:1, cs] = jnp.exp2(old - now[c])
                peak[head, 0:1, cs] = now[c]
            top = {}
            interleave(
                score_pieces(slot_n, head_n, 1 - k, top),
                weight_pieces(k, now),
                value_pieces(slot_p, head_p, 1 - k, factor_p),
            )
            keep_top(head_n, top)
        return (*slots[1], *slots[2])

    send_own(0)
    queries = (heads_of(0) * (1.4426950408889634 / HD**0.5)).astype(bf16)
    for h in range(4):
        qt[h] = queries[h * HD : (h + 1) * HD]
    w_own()
    top = {}
    for x in score_pieces(me, 0, 0, top):
        x()
    keep_top(0, top)
    lax.fori_loop(0, 32, step, (me, me * 0, me, me * 0))
    for x in value_pieces(slot_at(me * 0 + 15), 3, 1, {c: peak[5, 0:1, c * W : (c + 1) * W] for c in range(NC)}):
        x()
    finish((3,))
    relay(2)
    for c in loads[2:4]:
        c.wait()

    def project(c, _):
        cols = pl.ds(pl.multiple_of(c * W, W), W)
        mixed[cols, :] = tok[cols, :].astype(f32) + lax.dot_general(
            att[0:768, cols], wf[0:768, :], (((0,), (0,)), ((), ())), preferred_element_type=f32
        )
        return 0

    lax.fori_loop(0, NC, project, 0)
    relay(3)
    collect(2)
    collect(3)

    def complete(c, _):
        cols = pl.ds(pl.multiple_of(c * W, W), W)
        m = mixed[cols, :] + lax.dot_general(
            att[768:1536, cols], wf[768:1536, :], (((0,), (0,)), ((), ())), preferred_element_type=f32
        )
        mixed[cols, :] = m
        post[cols, :] = layer_norm(m, gain[...]).astype(bf16)
        return 0

    lax.fori_loop(0, NC, complete, 0)

    def rows_of(t, half=0, n=48):
        return pl.ds(pl.multiple_of(t * 96 + half * 48, 16), n)

    qsent = []

    def q_copy(src_ref, dst_ref, recv, dest, index):
        return pltpu.make_async_remote_copy(
            src_ref=src_ref, dst_ref=dst_ref, send_sem=qsend.at[index], recv_sem=recv,
            device_id={"tensor": dest}, device_id_type=MESH,
        )

    def q_start(src_ref, dst_ref, recv, dest):
        q_copy(src_ref, dst_ref, recv, dest, len(qsent)).start()
        qsent.append(0)

    def q_wait(ref, recv):
        q_copy(ref, ref, recv, ti, 0).wait_recv()

    def part(t, half):
        return term[rows_of(t, half), :].astype(f32)

    for dx in (2, 3, 1, 0):
        t0, t1 = ten_id(0, dx), ten_id(1, dx)
        both = jnp.concatenate([post[rows_of(t0, 0, 96), :], post[rows_of(t1, 0, 96), :]], axis=0)
        u = jnp.dot(both, wu[...], preferred_element_type=f32)
        h = jax.nn.gelu(u, approximate=True).astype(bf16)
        y = jnp.dot(h, wd[...], preferred_element_type=f32).astype(bf16)
        term[rows_of(t0, 0, 96), :] = y[0:96]
        term[rows_of(t1, 0, 96), :] = y[96:192]
        q_start(term.at[rows_of(t1, 1)], rb.at[dx], rbrecv.at[dx], ten_id(1, 0))
        if dx == 2:
            q_start(term.at[rows_of(t0)], rr.at[0], rrrecv.at[0], ten_id(0, 1))
            q_start(term.at[rows_of(t1)], rr.at[1], rrrecv.at[1], ten_id(0, 3))
        if dx == 1:
            q_start(term.at[rows_of(t1)], ra.at[1, 0], rarecv.at[1, 0], t0)
        if dx == 3:
            q_start(term.at[rows_of(t0)], ra.at[0, 1], rarecv.at[0, 1], t0)
    for k, dx in ((0, 1), (1, 3)):
        q_wait(rr.at[k], rrrecv.at[k])
        sr[k] = (part(ten_id(k, dx), 0) + rr[k].astype(f32)).astype(bf16)
        q_start(sr.at[k], ra.at[k, k], rarecv.at[k, k], ten_id(0, dx))
    for dx in (2, 1, 3):
        q_wait(rb.at[dx], rbrecv.at[dx])
        sb2[dx - 1] = (part(ten_id(0, dx), 1) + rb[dx].astype(f32)).astype(bf16)
        q_start(sb2.at[dx - 1], rb2.at[3 - dx], rb2recv.at[3 - dx], ten_id(0, dx))
    total = part(ten_id(1, 0), 0)
    for k in range(2):
        q_wait(ra.at[1, k], rarecv.at[1, k])
        total = total + ra[1, k].astype(f32)
    sa2[...] = total.astype(bf16)
    q_start(sa2, ra2, ra2recv.at[0], ten_id(1, 0))

    gsent = []

    def g_copy(t, half, dest, index):
        ref = out.at[rows_of(t, half)]
        return pltpu.make_async_remote_copy(
            src_ref=ref, dst_ref=ref, send_sem=gsend.at[index], recv_sem=grecv.at[t, half],
            device_id={"tensor": dest}, device_id_type=MESH,
        )

    def g_start(t, half, dest):
        g_copy(t, half, dest, len(gsent)).start()
        gsent.append(0)

    def g_wait(t, half):
        g_copy(t, half, ti, 0).wait_recv()

    q_wait(rb.at[0], rbrecv.at[0])
    total = mixed[rows_of(ti, 1), :] + part(ti, 1) + rb[0].astype(f32)
    for k in range(3):
        q_wait(rb2.at[k], rb2recv.at[k])
        total = total + rb2[k].astype(f32)
    out[rows_of(ti, 1), :] = total.astype(bf16)
    g_start(ti, 1, ten_id(1, 0))
    total = mixed[rows_of(ti, 0), :] + part(ti, 0)
    for k in range(2):
        q_wait(ra.at[0, k], rarecv.at[0, k])
        total = total + ra[0, k].astype(f32)
    q_wait(ra2, ra2recv.at[0])
    total = total + ra2[...].astype(f32)
    out[rows_of(ti, 0), :] = total.astype(bf16)
    for dx in (1, 3, 2):
        g_start(ti, 0, ten_id(0, dx))
    g_start(ti, 0, ten_id(1, 0))
    for dx in (1, 3):
        g_start(ti, 1, ten_id(0, dx))
    g_wait(ten_id(1, 0), 1)
    for dx in (1, 3):
        g_start(ten_id(1, 0), 1, ten_id(0, dx))
    for dx in (1, 3):
        g_wait(ten_id(0, dx), 0)
        g_start(ten_id(0, dx), 0, ten_id(1, 0))
    g_wait(ten_id(0, 3), 1)
    g_start(ten_id(0, 3), 1, ten_id(0, 1))
    g_wait(ten_id(0, 2), 0)
    g_start(ten_id(0, 2), 0, ten_id(1, 0))
    g_wait(ten_id(1, 1), 1)
    g_start(ten_id(1, 1), 1, ten_id(0, 3))
    g_wait(ten_id(1, 0), 0)
    for t, half in (((0, 1), 1), ((0, 2), 1), ((1, 3), 1), ((1, 2), 1), ((1, 1), 0), ((1, 3), 0), ((1, 2), 0)):
        g_wait(ten_id(*t), half)

    for hp in (0, 1):
        for index, piece in enumerate(sent[hp]):
            seq_copy(piece, me, hp, me, index).wait_send()
    for index in range(len(tsent)):
        ten_copy(ti, 0, ti, index).wait_send()
    for index in range(len(wsent)):
        w_copy(ti, 0, 0, {"tensor": ti}, index).wait_send()
    for index in range(len(qsent)):
        q_copy(sa2, ra2, ra2recv.at[0], ti, index).wait_send()
    for index in range(len(gsent)):
        g_copy(ti, 0, ti, index).wait_send()


def layer(gain_in, gain, tokens, w_in, w_out, w_up, w_down):
    vmem = pl.BlockSpec(memory_space=pltpu.VMEM)
    hbm = pl.BlockSpec(memory_space=pl.ANY)
    D = tokens.shape[1]
    return pl.pallas_call(
        layer_kernel,
        out_shape=jax.ShapeDtypeStruct((PAD, D), bf16),
        in_specs=[vmem, vmem, hbm, hbm, hbm, hbm, hbm],
        out_specs=vmem,
        scratch_shapes=[
            pltpu.VMEM((4, HD, PAD), bf16),
            pltpu.VMEM((3, 192, D), bf16),
            pltpu.VMEM((NSEQ, 4, HD, PAD), bf16),
            pltpu.VMEM((NSEQ, 4, 64, PAD), bf16),
            pltpu.VMEM((ROWS, PAD), f32),
            pltpu.VMEM((ROWS, PAD), f32),
            pltpu.VMEM((PAD, PAD), bf16),
            pltpu.VMEM((PAD, PAD), bf16),
            pltpu.VMEM((4, 64, PAD), f32),
            pltpu.VMEM((6, 16, PAD), f32),
            pltpu.VMEM((D, PAD), bf16),
            pltpu.VMEM((D, D), bf16),
            pltpu.VMEM((PAD, D), bf16),
            pltpu.VMEM((D, 768), bf16),
            pltpu.VMEM((768, D), bf16),
            pltpu.VMEM((PAD, D), f32),
            pltpu.VMEM((PAD, D), bf16),
            pltpu.VMEM((PAD, D), bf16),
            pltpu.VMEM((2, 2, 48, D), bf16),
            pltpu.VMEM((4, 48, D), bf16),
            pltpu.VMEM((48, D), bf16),
            pltpu.VMEM((3, 48, D), bf16),
            pltpu.VMEM((48, D), bf16),
            pltpu.VMEM((3, 48, D), bf16),
            pltpu.VMEM((2, 48, D), bf16),
            pltpu.VMEM((2, 48, D), bf16),
            pltpu.SemaphoreType.DMA((2, 32)),
            pltpu.SemaphoreType.DMA((NSEQ, 2, 2)),
            pltpu.SemaphoreType.DMA((32,)),
            pltpu.SemaphoreType.DMA((NTEN, 4)),
            pltpu.SemaphoreType.DMA((32,)),
            pltpu.SemaphoreType.DMA((NTEN, 2, 2)),
            pltpu.SemaphoreType.DMA((8,)),
            pltpu.SemaphoreType.DMA((16,)),
            pltpu.SemaphoreType.DMA((2, 2)),
            pltpu.SemaphoreType.DMA((4,)),
            pltpu.SemaphoreType.DMA((1,)),
            pltpu.SemaphoreType.DMA((3,)),
            pltpu.SemaphoreType.DMA((2,)),
            pltpu.SemaphoreType.DMA((16,)),
            pltpu.SemaphoreType.DMA((NTEN, 2)),
        ],
        compiler_params=pltpu.CompilerParams(
            collective_id=0, has_side_effects=True, vmem_limit_bytes=60 * 2**20,
        ),
        cost_estimate=pl.CostEstimate(flops=60_000_000_000, bytes_accessed=4_000_000, transcendentals=33_000_000),
        name="layer",
    )(gain_in, gain, tokens, w_in, w_out, w_up, w_down)


def per_device(tokens, norm_gain, w_qkv, w_out, post_gain, w_up, w_down):
    w_in = jnp.transpose(w_qkv, (1, 2, 0))
    return layer(norm_gain[None, :], post_gain[None, :], tokens, w_in, w_out, w_up, w_down)[:ROWS]


def solution(mesh):
    placed = (P("seq", None), P(), P(None, None, "tensor"), P("tensor", None), P(), P(None, "tensor"), P("tensor", None))
    return jax.shard_map(per_device, mesh=mesh, in_specs=placed, out_specs=P("seq", None), check_vma=False)
```

```python
import functools

import jax
import jax.numpy as jnp
from jax import lax
from jax.experimental import pallas as pl
from jax.experimental.pallas import tpu as pltpu
from jax.sharding import PartitionSpec as P

HD = 48
ROWS = 720
PAD = 768
NSEQ = 16
NTEN = 8
W = 256
NC = PAD // W
f32 = jnp.float32
bf16 = jnp.bfloat16
MESH = pl.DeviceIdType.MESH

OWN, A, B, C, F, D, E, G = range(8)
DZ = (0, 0, 0, 1, 0, 1, 1, 1)
DY = (0, 3, 1, 0, 2, 3, 1, 2)
ARRIVE = {
    0: ((0, OWN, 1),), 4: ((0, A, 1),), 5: ((0, B, 1),), 6: ((0, C, 1), (0, D, 0), (0, E, 0)),
    9: ((0, D, 1), (0, F, 0)), 10: ((0, E, 1),), 12: ((0, G, 0),), 13: ((0, F, 1),), 14: ((0, G, 1),),
    15: ((1, OWN, 1),), 16: ((1, A, 0), (1, B, 0), (1, C, 0)), 20: ((1, A, 1),), 21: ((1, B, 1), (1, D, 0), (1, E, 0)),
    22: ((1, C, 1),), 23: ((1, D, 1),), 24: ((1, E, 1), (1, F, 0)), 25: ((1, G, 0), (1, F, 1)), 26: ((1, G, 1),),
}


def layer_norm(values, gain):
    mean = jnp.mean(values, axis=-1, keepdims=True)
    centred = values - mean
    var = jnp.mean(centred * centred, axis=-1, keepdims=True)
    return centred * lax.rsqrt(var + 1e-05) * gain


def layer_kernel(gain_in, gain, tokens, w_in, w_out, w_up, w_down, out, qt, wq, kt, vt, s0, s1, p0, p1, acc, peak, att, wf, tok, wu, wd,
                 mixed, post, term, ra, rb, ra2, rb2, sa2, sb2, rr, sr, ssem, rsem, tsend, trecv, wsend, wrecv, lsem,
                 qsend, rarecv, rbrecv, ra2recv, rb2recv, rrrecv, gsend, grecv):
    me = lax.axis_index("seq")
    ti = lax.axis_index("tensor")
    zh, yy, core = lax.div(me, 8), lax.rem(lax.div(me, 2), 4), lax.rem(me, 2)
    zl, xx = lax.div(ti, 4), lax.rem(ti, 4)

    def seq_id(off, other=0):
        return (lax.rem(zh + DZ[off], 2) * 4 + lax.rem(yy + DY[off], 4)) * 2 + lax.rem(core + other, 2)

    def ten_id(dz, dx):
        return lax.rem(zl + dz, 2) * 4 + lax.rem(xx + dx, 4)

    seq_near = [seq_id(OWN, 1), seq_id(A), seq_id(B), seq_id(C)]
    ten_near = [ten_id(0, 1), ten_id(0, 3), ten_id(1, 0), ten_id(1, 1), ten_id(1, 3)]
    ten_all = [ten_id(0, 1), ten_id(0, 3), ten_id(0, 2), ten_id(1, 0), ten_id(1, 1), ten_id(1, 3)]
    loads = [
        pltpu.make_async_copy(tokens, tok.at[0:ROWS], lsem.at[0]),
        pltpu.make_async_copy(w_in, wq, lsem.at[1]),
        pltpu.make_async_copy(w_up, wu, lsem.at[2]),
        pltpu.make_async_copy(w_down, wd, lsem.at[3]),
    ]
    loads += [
        pltpu.make_async_copy(
            w_out.at[h * HD : (h + 1) * HD], wf.at[pl.ds(pl.multiple_of(h * 384 + ti * HD, 16), HD)], lsem.at[4 + h]
        )
        for h in range(4)
    ]
    for c in loads:
        c.start()
    barrier = pltpu.get_barrier_semaphore()
    for d in seq_near:
        pl.semaphore_signal(barrier, inc=1, device_id={"seq": d}, device_id_type=MESH)
    for d in ten_all:
        pl.semaphore_signal(barrier, inc=1, device_id={"tensor": d}, device_id_type=MESH)

    lane = lax.broadcasted_iota(jnp.int32, (16, PAD), 1)
    row = lax.broadcasted_iota(jnp.int32, (16, PAD), 0)
    ones = jnp.where((row == 0) & (lane < ROWS), 1.0, 0.0).astype(bf16)

    def fill(s, _):
        for h in range(4):
            vt[s, h, HD:64, :] = ones
        return 0

    lax.fori_loop(0, NSEQ, fill, 0)
    peak[0:4] = jnp.full((4, 16, PAD), -1e30, f32)
    peak[4:6] = jnp.ones((2, 16, PAD), f32)
    acc[...] = jnp.zeros(acc.shape, f32)
    p0[ROWS:PAD, :] = jnp.zeros((PAD - ROWS, PAD), bf16)
    p1[...] = jnp.zeros((PAD, PAD), bf16)
    tok[ROWS:PAD, :] = jnp.zeros((PAD - ROWS, 1536), bf16)
    loads[0].wait()

    def norm(c, _):
        rows = pl.ds(pl.multiple_of(c * W, W), W)
        post[rows, :] = layer_norm(tok[rows, :].astype(f32), gain_in[...]).astype(bf16)
        return 0

    lax.fori_loop(0, NC, norm, 0)
    loads[1].wait()

    def heads_of(part):
        return lax.dot_general(wq[part], post[...], (((1,), (1,)), ((), ())), preferred_element_type=f32)

    keys = heads_of(1).astype(bf16)
    values = heads_of(2).astype(bf16)
    for h in range(4):
        kt[me, h] = keys[h * HD : (h + 1) * HD]
        vt[me, h, 0:HD, :] = values[h * HD : (h + 1) * HD]
    pl.semaphore_wait(barrier, len(seq_near) + len(ten_all))

    sent = [[], []]

    def block_ref(piece, slot, hp):
        ref = kt if piece == 0 else vt
        return ref.at[slot, 2 * hp : 2 * hp + 2, 0:HD]

    def seq_copy(piece, slot, hp, dest, index):
        return pltpu.make_async_remote_copy(
            src_ref=block_ref(piece, slot, hp), dst_ref=block_ref(piece, slot, hp), send_sem=ssem.at[hp, index],
            recv_sem=rsem.at[slot, hp, piece], device_id={"seq": dest}, device_id_type=MESH,
        )

    def send(piece, slot, hp, dest):
        c = seq_copy(piece, slot, hp, dest, len(sent[hp]))
        c.start()
        sent[hp].append(piece)

    def send_own(hp):
        for piece in (0, 1):
            for d in (seq_id(B), seq_id(A), seq_id(C), seq_id(OWN, 1)):
                send(piece, me, hp, d)

    def arrive(hp, off, other, pieces=(0, 1)):
        slot = seq_id(off, other)
        for piece in pieces:
            seq_copy(piece, slot, hp, me, 0).wait_recv()
        if other:
            return
        if off in (D, E):
            onward(hp, off)
        for piece in pieces:
            send(piece, slot, hp, seq_id(OWN, 1))

    def onward(hp, off):
        if off in (A, D):
            send(0, seq_id(off), hp, seq_id(B))
        else:
            send(1, seq_id(off), hp, seq_id(A))

    def spread(hp, pieces=(0, 1)):
        slot = seq_id(C)
        for piece in pieces:
            for d in (seq_id(B), seq_id(A)):
                send(piece, slot, hp, d)
        for piece in pieces:
            onward(hp, (A, B)[piece])

    tsent = []

    def head_ref(src, head):
        return att.at[pl.ds(pl.multiple_of(head * 384 + src * HD, 16), HD)]

    def ten_copy(src, head, dest, index):
        return pltpu.make_async_remote_copy(
            src_ref=head_ref(src, head), dst_ref=head_ref(src, head), send_sem=tsend.at[index],
            recv_sem=trecv.at[src, head], device_id={"tensor": dest}, device_id_type=MESH,
        )

    def ten_start(src, head, dest):
        c = ten_copy(src, head, dest, len(tsent))
        c.start()
        tsent.append(0)

    def finish(heads):
        for h in heads:
            att[pl.ds(pl.multiple_of(h * 384 + ti * HD, 16), HD), :] = (acc[h, 0:HD, :] / acc[h, HD : HD + 1, :]).astype(bf16)
        for h in heads:
            for d in ten_near:
                ten_start(ti, h, d)

    def ten_wait(src, head):
        ten_copy(src, head, ti, 0).wait_recv()

    def relay(head):
        for src, dest in ((ten_id(0, 3), ten_id(0, 1)), (ten_id(1, 1), ten_id(0, 3))):
            ten_wait(src, head)
            ten_start(src, head, dest)

    def collect(head):
        for src in (ten_id(0, 1), ten_id(1, 3), ten_id(1, 0), ten_id(0, 2), ten_id(1, 2)):
            ten_wait(src, head)

    wsent = []

    def w_copy(src, half, other, dest, index):
        at = lax.rem(core + other, 2)
        ref = wf.at[pl.ds(pl.multiple_of((at * 2 + half) * 384 + src * HD, 16), HD)]
        return pltpu.make_async_remote_copy(
            src_ref=ref, dst_ref=ref, send_sem=wsend.at[index], recv_sem=wrecv.at[src, other, half],
            device_id=dest, device_id_type=MESH,
        )

    def w_start(src, half, dest, index_other=0):
        at = core
        ref = wf.at[pl.ds(pl.multiple_of((at * 2 + half) * 384 + src * HD, 16), HD)]
        pltpu.make_async_remote_copy(
            src_ref=ref, dst_ref=ref, send_sem=wsend.at[len(wsent)], recv_sem=wrecv.at[src, index_other, half],
            device_id=dest, device_id_type=MESH,
        ).start()
        wsent.append(0)

    def w_wait(src, half, other):
        w_copy(src, half, other, {"tensor": ti}, 0).wait_recv()

    def w_share(src):
        for half in (0, 1):
            w_start(src, half, {"seq": seq_id(OWN, 1)}, 1)

    def w_own():
        for c in loads[4:]:
            c.wait()
        for half in (0, 1):
            for d in (ten_id(0, 1), ten_id(0, 3), ten_id(1, 0)):
                w_start(ti, half, {"tensor": d})

    def w_relay(dz):
        left, right = ten_id(dz, 3), ten_id(dz, 1)
        for src in (left, right):
            for half in (0, 1):
                w_wait(src, half, 0)
        w_start(left, 0, {"tensor": ten_id(0, 1)})
        w_start(right, 1, {"tensor": ten_id(0, 3)})
        w_share(left)
        w_share(right)

    def w_cross():
        src = ten_id(1, 0)
        for half in (0, 1):
            w_wait(src, half, 0)
            for d in (ten_id(0, 1), ten_id(0, 3)):
                w_start(src, half, {"tensor": d})
        w_share(src)

    def w_far(dz):
        src = ten_id(dz, 2)
        for half in (0, 1):
            w_wait(src, half, 0)
        w_share(src)

    def w_collect():
        for dz in (0, 1):
            for dx in range(4):
                if (dz, dx) != (0, 0):
                    for half in (0, 1):
                        w_wait(ten_id(dz, dx), half, 1)

    S, Pw = (s0, s1), (p0, p1)

    def slot_at(pos):
        mid, late = (pos >= 2).astype(jnp.int32), (pos >= 8).astype(jnp.int32)
        q, r = lax.rem(pos + 4, 6), lax.rem(pos, 4)
        chip = mid * (1 - late) * (1 + lax.rem(q, 3)) + late * (2 * lax.div(pos, 4) + lax.rem(r, 2))
        other = (1 - mid) * pos + mid * (1 - late) * lax.div(q, 3) + late * lax.div(r, 2)
        far = (chip >= 6).astype(jnp.int32)
        dy = (1 - far) * lax.rem(3 * lax.rem(chip, 3), 5) + 2 * far
        dz = (1 - far) * lax.div(chip, 3) + far * (chip - 6)
        return (lax.rem(zh + dz, 2) * 4 + lax.rem(yy + dy, 4)) * 2 + lax.rem(core + other, 2)

    def score_pieces(slot, head, par, top):
        def mk(c, half):
            cs = slice(c * W, (c + 1) * W)

            def go():
                lo = half * 384
                n = 384 if half == 0 else ROWS - 384
                s = lax.dot_general(
                    kt[slot, head, :, lo : lo + 384], qt[head, :, cs], (((0,), (0,)), ((), ())), preferred_element_type=f32
                )[0:n]
                S[par][lo : lo + n, cs] = s
                b = jnp.max(s.reshape(-1, 8, W), axis=0)
                top[c] = b if c not in top else jnp.maximum(top[c], b)

            return go

        return [mk(c, half) for c in range(NC) for half in (0, 1)]

    def weight_pieces(par, now):
        def mk(c, r):
            cs = slice(c * W, (c + 1) * W)

            def go():
                Pw[par][r : r + 240, cs] = jnp.exp2(S[par][r : r + 240, cs] - now[c]).astype(bf16)

            return go

        return [mk(c, r) for c in range(NC) for r in (0, 240, 480)]

    def value_pieces(slot, head, par, factor):
        def mk(c):
            cs = slice(c * W, (c + 1) * W)

            def go():
                acc[head, :, cs] = acc[head, :, cs] * factor[c] + jnp.dot(
                    vt[slot, head], Pw[par][:, cs], preferred_element_type=f32
                )

            return go

        return [mk(c) for c in range(NC)]

    def interleave(*lists):
        events = []
        for k, items in enumerate(lists):
            for j, x in enumerate(items):
                events.append(((j + 0.5) / len(items), k, x))
        events.sort(key=lambda e: (e[0], e[1]))
        for _, _, x in events:
            x()

    def keep_top(head, top):
        for c in range(NC):
            peak[head, 8:16, c * W : (c + 1) * W] = top[c]

    def item(n):
        n = lax.rem(n, 64)
        late = (n >= 44).astype(jnp.int32)
        last = (n >= 54).astype(jnp.int32)
        pos = (1 - late) * lax.div(lax.rem(n, 32), 2) + late * (n - 38 - 10 * last)
        head = (1 - late) * (2 * lax.div(n, 32) + lax.rem(n, 2)) + late * (2 + last)
        return slot_at(pos), head

    def step(t, held):
        def events(at):
            for hp, off, other in ARRIVE.get(at, ()):
                arrive(hp, off, other)
            if at in (1, 2):
                for off in (A, B, C):
                    arrive(0, off, 0, (at - 1,))
                spread(0, (at - 1,))
            if at == 4:
                w_cross()
                w_relay(0)
            if at == 7:
                send_own(1)
            if at == 12:
                w_relay(1)
                w_far(0)
            if at == 15:
                w_far(1)
            if at == 16:
                spread(1)
            if at == 17:
                finish((0, 1))
            if at == 24:
                relay(0)
                relay(1)
            if at == 30:
                collect(0)
                collect(1)
                w_collect()
            if at == 28:
                finish((2,))

        at_all = sorted(set(ARRIVE) | {1, 2, 4, 7, 12, 15, 16, 17, 24, 28, 30})

        def search(lo, hi):
            inside = [at for at in at_all if lo <= at < hi]
            if not inside:
                return
            if hi - lo == 1:
                events(lo)
                return
            mid = (lo + hi) // 2
            for a, b in ((lo, mid), (mid, hi)):
                if any(a <= at < b for at in inside):
                    test = t < mid if a == lo else t >= mid
                    pl.when(test)(functools.partial(search, a, b))

        search(0, 32)
        slots = {q: item(2 * t + q) for q in (1, 2)}
        slots[-1], slots[0] = (held[0], held[1]), (held[2], held[3])
        for k in (0, 1):
            (slot_p, head_p), (slot, head), (slot_n, head_n) = slots[k - 1], slots[k], slots[k + 1]
            now, factor_p = {}, {}
            for c in range(NC):
                cs = slice(c * W, (c + 1) * W)
                factor_p[c] = peak[5 - k, 0:1, cs]
                old = peak[head, 0:1, cs]
                now[c] = jnp.maximum(old, jnp.max(peak[head, 8:16, cs], axis=0, keepdims=True))
                peak[4 + k, 0:1, cs] = jnp.exp2(old - now[c])
                peak[head, 0:1, cs] = now[c]
            top = {}
            interleave(
                score_pieces(slot_n, head_n, 1 - k, top),
                weight_pieces(k, now),
                value_pieces(slot_p, head_p, 1 - k, factor_p),
            )
            keep_top(head_n, top)
        return (*slots[1], *slots[2])

    send_own(0)
    queries = (heads_of(0) * (1.4426950408889634 / HD**0.5)).astype(bf16)
    for h in range(4):
        qt[h] = queries[h * HD : (h + 1) * HD]
    w_own()
    top = {}
    for x in score_pieces(me, 0, 0, top):
        x()
    keep_top(0, top)
    lax.fori_loop(0, 32, step, (me, me * 0, me, me * 0))
    for x in value_pieces(slot_at(me * 0 + 15), 3, 1, {c: peak[5, 0:1, c * W : (c + 1) * W] for c in range(NC)}):
        x()
    finish((3,))
    relay(2)
    for c in loads[2:4]:
        c.wait()

    def project(c, _):
        cols = pl.ds(pl.multiple_of(c * W, W), W)
        mixed[cols, :] = tok[cols, :].astype(f32) + lax.dot_general(
            att[0:768, cols], wf[0:768, :], (((0,), (0,)), ((), ())), preferred_element_type=f32
        )
        return 0

    lax.fori_loop(0, NC, project, 0)
    relay(3)
    collect(2)
    collect(3)

    def complete(c, _):
        cols = pl.ds(pl.multiple_of(c * W, W), W)
        m = mixed[cols, :] + lax.dot_general(
            att[768:1536, cols], wf[768:1536, :], (((0,), (0,)), ((), ())), preferred_element_type=f32
        )
        mixed[cols, :] = m
        post[cols, :] = layer_norm(m, gain[...]).astype(bf16)
        return 0

    lax.fori_loop(0, NC, complete, 0)

    def rows_of(t, half=0, n=48):
        return pl.ds(pl.multiple_of(t * 96 + half * 48, 16), n)

    qsent = []

    def q_copy(src_ref, dst_ref, recv, dest, index):
        return pltpu.make_async_remote_copy(
            src_ref=src_ref, dst_ref=dst_ref, send_sem=qsend.at[index], recv_sem=recv,
            device_id={"tensor": dest}, device_id_type=MESH,
        )

    def q_start(src_ref, dst_ref, recv, dest):
        q_copy(src_ref, dst_ref, recv, dest, len(qsent)).start()
        qsent.append(0)

    def q_wait(ref, recv):
        q_copy(ref, ref, recv, ti, 0).wait_recv()

    def part(t, half):
        return term[rows_of(t, half), :].astype(f32)

    for dx in (2, 3, 1, 0):
        t0, t1 = ten_id(0, dx), ten_id(1, dx)
        both = jnp.concatenate([post[rows_of(t0, 0, 96), :], post[rows_of(t1, 0, 96), :]], axis=0)
        u = jnp.dot(both, wu[...], preferred_element_type=f32)
        h = jax.nn.gelu(u, approximate=True).astype(bf16)
        y = jnp.dot(h, wd[...], preferred_element_type=f32).astype(bf16)
        term[rows_of(t0, 0, 96), :] = y[0:96]
        term[rows_of(t1, 0, 96), :] = y[96:192]
        q_start(term.at[rows_of(t1, 1)], rb.at[dx], rbrecv.at[dx], ten_id(1, 0))
        if dx == 2:
            q_start(term.at[rows_of(t0)], rr.at[0], rrrecv.at[0], ten_id(0, 1))
            q_start(term.at[rows_of(t1)], rr.at[1], rrrecv.at[1], ten_id(0, 3))
        if dx == 1:
            q_start(term.at[rows_of(t1)], ra.at[1, 0], rarecv.at[1, 0], t0)
        if dx == 3:
            q_start(term.at[rows_of(t0)], ra.at[0, 1], rarecv.at[0, 1], t0)
    for k, dx in ((0, 1), (1, 3)):
        q_wait(rr.at[k], rrrecv.at[k])
        sr[k] = (part(ten_id(k, dx), 0) + rr[k].astype(f32)).astype(bf16)
        q_start(sr.at[k], ra.at[k, k], rarecv.at[k, k], ten_id(0, dx))
    for dx in (2, 1, 3):
        q_wait(rb.at[dx], rbrecv.at[dx])
        sb2[dx - 1] = (part(ten_id(0, dx), 1) + rb[dx].astype(f32)).astype(bf16)
        q_start(sb2.at[dx - 1], rb2.at[3 - dx], rb2recv.at[3 - dx], ten_id(0, dx))
    total = part(ten_id(1, 0), 0)
    for k in range(2):
        q_wait(ra.at[1, k], rarecv.at[1, k])
        total = total + ra[1, k].astype(f32)
    sa2[...] = total.astype(bf16)
    q_start(sa2, ra2, ra2recv.at[0], ten_id(1, 0))

    gsent = []

    def g_copy(t, half, dest, index):
        ref = out.at[rows_of(t, half)]
        return pltpu.make_async_remote_copy(
            src_ref=ref, dst_ref=ref, send_sem=gsend.at[index], recv_sem=grecv.at[t, half],
            device_id={"tensor": dest}, device_id_type=MESH,
        )

    def g_start(t, half, dest):
        g_copy(t, half, dest, len(gsent)).start()
        gsent.append(0)

    def g_wait(t, half):
        g_copy(t, half, ti, 0).wait_recv()

    q_wait(rb.at[0], rbrecv.at[0])
    total = mixed[rows_of(ti, 1), :] + part(ti, 1) + rb[0].astype(f32)
    for k in range(3):
        q_wait(rb2.at[k], rb2recv.at[k])
        total = total + rb2[k].astype(f32)
    out[rows_of(ti, 1), :] = total.astype(bf16)
    g_start(ti, 1, ten_id(1, 0))
    total = mixed[rows_of(ti, 0), :] + part(ti, 0)
    for k in range(2):
        q_wait(ra.at[0, k], rarecv.at[0, k])
        total = total + ra[0, k].astype(f32)
    q_wait(ra2, ra2recv.at[0])
    total = total + ra2[...].astype(f32)
    out[rows_of(ti, 0), :] = total.astype(bf16)
    for dx in (1, 3, 2):
        g_start(ti, 0, ten_id(0, dx))
    g_start(ti, 0, ten_id(1, 0))
    for dx in (1, 3):
        g_start(ti, 1, ten_id(0, dx))
    g_wait(ten_id(1, 0), 1)
    for dx in (1, 3):
        g_start(ten_id(1, 0), 1, ten_id(0, dx))
    for dx in (1, 3):
        g_wait(ten_id(0, dx), 0)
        g_start(ten_id(0, dx), 0, ten_id(1, 0))
    g_wait(ten_id(0, 3), 1)
    g_start(ten_id(0, 3), 1, ten_id(0, 1))
    g_wait(ten_id(0, 2), 0)
    g_start(ten_id(0, 2), 0, ten_id(1, 0))
    g_wait(ten_id(1, 1), 1)
    g_start(ten_id(1, 1), 1, ten_id(0, 3))
    g_wait(ten_id(1, 0), 0)
    for t, half in (((0, 1), 1), ((0, 2), 1), ((1, 3), 1), ((1, 2), 1), ((1, 1), 0), ((1, 3), 0), ((1, 2), 0)):
        g_wait(ten_id(*t), half)

    for hp in (0, 1):
        for index, piece in enumerate(sent[hp]):
            seq_copy(piece, me, hp, me, index).wait_send()
    for index in range(len(tsent)):
        ten_copy(ti, 0, ti, index).wait_send()
    for index in range(len(wsent)):
        w_copy(ti, 0, 0, {"tensor": ti}, index).wait_send()
    for index in range(len(qsent)):
        q_copy(sa2, ra2, ra2recv.at[0], ti, index).wait_send()
    for index in range(len(gsent)):
        g_copy(ti, 0, ti, index).wait_send()


def layer(gain_in, gain, tokens, w_in, w_out, w_up, w_down):
    vmem = pl.BlockSpec(memory_space=pltpu.VMEM)
    hbm = pl.BlockSpec(memory_space=pl.ANY)
    D = tokens.shape[1]
    return pl.pallas_call(
        layer_kernel,
        out_shape=jax.ShapeDtypeStruct((PAD, D), bf16),
        in_specs=[vmem, vmem, hbm, hbm, hbm, hbm, hbm],
        out_specs=vmem,
        scratch_shapes=[
            pltpu.VMEM((4, HD, PAD), bf16),
            pltpu.VMEM((3, 192, D), bf16),
            pltpu.VMEM((NSEQ, 4, HD, PAD), bf16),
            pltpu.VMEM((NSEQ, 4, 64, PAD), bf16),
            pltpu.VMEM((ROWS, PAD), f32),
            pltpu.VMEM((ROWS, PAD), f32),
            pltpu.VMEM((PAD, PAD), bf16),
            pltpu.VMEM((PAD, PAD), bf16),
            pltpu.VMEM((4, 64, PAD), f32),
            pltpu.VMEM((6, 16, PAD), f32),
            pltpu.VMEM((D, PAD), bf16),
            pltpu.VMEM((D, D), bf16),
            pltpu.VMEM((PAD, D), bf16),
            pltpu.VMEM((D, 768), bf16),
            pltpu.VMEM((768, D), bf16),
            pltpu.VMEM((PAD, D), f32),
            pltpu.VMEM((PAD, D), bf16),
            pltpu.VMEM((PAD, D), bf16),
            pltpu.VMEM((2, 2, 48, D), bf16),
            pltpu.VMEM((4, 48, D), bf16),
            pltpu.VMEM((48, D), bf16),
            pltpu.VMEM((3, 48, D), bf16),
            pltpu.VMEM((48, D), bf16),
            pltpu.VMEM((3, 48, D), bf16),
            pltpu.VMEM((2, 48, D), bf16),
            pltpu.VMEM((2, 48, D), bf16),
            pltpu.SemaphoreType.DMA((2, 32)),
            pltpu.SemaphoreType.DMA((NSEQ, 2, 2)),
            pltpu.SemaphoreType.DMA((32,)),
            pltpu.SemaphoreType.DMA((NTEN, 4)),
            pltpu.SemaphoreType.DMA((32,)),
            pltpu.SemaphoreType.DMA((NTEN, 2, 2)),
            pltpu.SemaphoreType.DMA((8,)),
            pltpu.SemaphoreType.DMA((16,)),
            pltpu.SemaphoreType.DMA((2, 2)),
            pltpu.SemaphoreType.DMA((4,)),
            pltpu.SemaphoreType.DMA((1,)),
            pltpu.SemaphoreType.DMA((3,)),
            pltpu.SemaphoreType.DMA((2,)),
            pltpu.SemaphoreType.DMA((16,)),
            pltpu.SemaphoreType.DMA((NTEN, 2)),
        ],
        compiler_params=pltpu.CompilerParams(
            collective_id=0, has_side_effects=True, vmem_limit_bytes=60 * 2**20,
        ),
        cost_estimate=pl.CostEstimate(flops=60_000_000_000, bytes_accessed=4_000_000, transcendentals=33_000_000),
        name="layer",
    )(gain_in, gain, tokens, w_in, w_out, w_up, w_down)


def per_device(tokens, norm_gain, w_qkv, w_out, post_gain, w_up, w_down):
    w_in = jnp.transpose(w_qkv, (1, 2, 0))
    return layer(norm_gain[None, :], post_gain[None, :], tokens, w_in, w_out, w_up, w_down)[:ROWS]


def solution(mesh):
    placed = (P("seq", None), P(), P(None, None, "tensor"), P("tensor", None), P(), P(None, "tensor"), P("tensor", None))
    return jax.shard_map(per_device, mesh=mesh, in_specs=placed, out_specs=P("seq", None), check_vma=False)
```
